32 devices in a mesh: dp: 1 (over z), tp2: 4 (over y), tp: 8 (over x, core).
Axes of the slice: x: 4, y: 4, z: 1, core: 2. Of those that a mesh axis runs over, the one named last changes fastest.
The devices are a block of a 4x4x8 slice.
Arguments:
- hidden: bfloat16 [512, 2304], P('dp')
- w_gate: bfloat16 [2304, 9216], P(None, ('tp2', 'tp'))
- w_up: bfloat16 [2304, 9216], P(None, ('tp2', 'tp'))
- w_down: bfloat16 [9216, 2304], P(('tp2', 'tp'))
- norm_gain: float32 [2304], replicated
- w_vocab: bfloat16 [2304, 256000], P(None, ('tp2', 'tp'))
- temperature: float32 [512], P('dp')
- target_ids: int32 [512], P('dp')
Outputs:
- output 1: float32 [512], P('dp')
- output 2: float32 [512], P('dp')
- output 3: float32 [512], P('dp')
- output 4: bfloat16 [512, 256000], P('dp', ('tp2', 'tp'))
All inputs are finite; a program needn't handle non-finite values.
Results may differ from the reference program's by a relative error of at most 0.00381759.
Values are sent between devices in bfloat16 or wider.
A program may use at most 768 MiB of HBM per device.

```python
import jax
import jax.numpy as jnp
from jax import lax

BATCH_ROWS = 512
D_MODEL = 2304
D_FF = 9216
VOCAB_SIZE = 256000
ROW_BLOCK = 8
NORM_EPS = 1e-6


def setup_inputs(seed: int = 0, part: int = 0) -> dict:
    base_key = jax.random.key(seed)
    part_key = jax.random.fold_in(base_key, part)
    shared = jax.random.split(base_key, 6)
    own_keys = jax.random.split(part_key, 3)
    hidden = jax.random.normal(own_keys[0], (BATCH_ROWS, D_MODEL), jnp.float32)
    w_gate = jax.random.normal(shared[0], (D_MODEL, D_FF), jnp.float32) * D_MODEL ** -0.5
    w_up = jax.random.normal(shared[1], (D_MODEL, D_FF), jnp.float32) * D_MODEL ** -0.5
    w_down = jax.random.normal(shared[2], (D_FF, D_MODEL), jnp.float32) * (2.0 * D_FF ** -0.5)
    norm_gain = jax.random.uniform(shared[3], (D_MODEL,), jnp.float32, 0.5, 1.5)
    col_scale = jnp.exp(0.3 * jax.random.normal(shared[4], (1, VOCAB_SIZE), jnp.float32))
    w_vocab = jax.random.normal(shared[5], (D_MODEL, VOCAB_SIZE), jnp.float32) * D_MODEL ** -0.5 * col_scale
    temperature = jax.random.uniform(own_keys[1], (BATCH_ROWS,), jnp.float32, 0.5, 2.0)
    target_ids = jax.random.randint(own_keys[2], (BATCH_ROWS,), 0, VOCAB_SIZE, jnp.int32)
    return {
        'hidden': hidden.astype(jnp.bfloat16),
        'w_gate': w_gate.astype(jnp.bfloat16),
        'w_up': w_up.astype(jnp.bfloat16),
        'w_down': w_down.astype(jnp.bfloat16),
        'norm_gain': norm_gain,
        'w_vocab': w_vocab.astype(jnp.bfloat16),
        'temperature': temperature,
        'target_ids': target_ids,
    }


def reference(hidden, w_gate, w_up, w_down, norm_gain, w_vocab, temperature, target_ids):
    gate_pre = jnp.dot(hidden, w_gate, preferred_element_type=jnp.float32)
    up_pre = jnp.dot(hidden, w_up, preferred_element_type=jnp.float32)
    hidden_act = (jax.nn.silu(gate_pre) * up_pre).astype(jnp.bfloat16)
    mlp_out = jnp.dot(hidden_act, w_down, preferred_element_type=jnp.float32).astype(jnp.bfloat16)
    resid_sum = hidden.astype(jnp.float32) + mlp_out.astype(jnp.float32)
    inv_rms = lax.rsqrt(jnp.mean(resid_sum * resid_sum, axis=-1, keepdims=True) + NORM_EPS)
    normed = (norm_gain * resid_sum * inv_rms).astype(jnp.bfloat16)
    num_blocks = BATCH_ROWS // ROW_BLOCK

    def head_block(block_in):
        block_x, block_temp, block_ids = block_in
        logits = jnp.dot(block_x, w_vocab, preferred_element_type=jnp.float32) / block_temp[:, None]
        row_max = jnp.max(logits, axis=-1, keepdims=True)
        shifted = jnp.exp(logits - row_max)
        sum_exp = jnp.sum(shifted, axis=-1)
        log_norm = row_max[:, 0] + jnp.log(sum_exp)
        mean_logit = jnp.sum(shifted * logits, axis=-1) / sum_exp
        target_logit = jnp.take_along_axis(logits, block_ids[:, None], axis=-1)[:, 0]
        logprobs = (logits - log_norm[:, None]).astype(jnp.bfloat16)
        return log_norm, log_norm - mean_logit, target_logit - log_norm, logprobs

    log_norm, entropy, target_logp, logprobs = lax.map(
        head_block,
        (normed.reshape(num_blocks, ROW_BLOCK, D_MODEL),
         temperature.reshape(num_blocks, ROW_BLOCK),
         target_ids.reshape(num_blocks, ROW_BLOCK)))
    return (log_norm.reshape(BATCH_ROWS), entropy.reshape(BATCH_ROWS),
            target_logp.reshape(BATCH_ROWS), logprobs.reshape(BATCH_ROWS, VOCAB_SIZE))
```

```python
import jax
import jax.numpy as jnp
from jax import lax
from jax.experimental import pallas as pl
from jax.experimental.pallas import tpu as pltpu
from jax.sharding import PartitionSpec as P

NORM_EPS = 1e-6
CORES = 2
CHUNKS = 2
BLOCKS = 10
MESH = pl.DeviceIdType.MESH
NT = (((1,), (1,)), ((), ()))
F32, BF16 = jnp.float32, jnp.bfloat16


def split(start, stop, pieces):
    step = -(-(stop - start) // pieces)
    step = -(-step // 16) * 16
    return [(i, min(step, stop - i)) for i in range(start, stop, step)]


def main_kernel(n2, n1, hid, hid3, wg, wu, wd, gain, wvt, temp, tid, lg, stats,
                wv, yp, d0, st1, st2, xf, xm, hs, act, so, sr,
                load_sem, hs_sem, s0_s, s0_r, s1_s, s1_r, s2_s, s2_r,
                ga_s, gb_s, gc_s, g_r, so_s, so_r):
    group = n1 * n2
    half = group // CORES
    rows, width = hid.shape
    ff = wg.shape[0]
    vocab = wvt.shape[0]
    chunk = rows // CHUNKS
    block = vocab // BLOCKS

    y = lax.axis_index('tp2')
    t = lax.axis_index('tp')
    core = lax.rem(t, CORES)
    x = lax.div(t, CORES)
    me = y * n1 + t
    f = x + core * (y - x)
    s = y + core * (x - y)
    mine = core * half + f * n2 + s

    def dev(a, b):
        return {'tp2': b + core * (a - b), 'tp': CORES * (a + core * (b - a)) + core}

    partner = {'tp2': y, 'tp': CORES * x + (1 - core)}

    def slab(a, b):
        return core * half + a * n2 + b

    def other(k):
        i = lax.rem(me + k, group)
        return {'tp2': lax.div(i, n1), 'tp': lax.rem(i, n1)}

    def remote(src, dst, ssem, rsem, to):
        return pltpu.make_async_remote_copy(src_ref=src, dst_ref=dst, send_sem=ssem, recv_sem=rsem,
                                            device_id=to, device_id_type=MESH)

    h0 = vocab - 3 * ff - rows
    g0, d_0 = h0 + rows, h0 + rows + 2 * ff
    first = [(hid.at[pl.ds(0, chunk)], wv.at[pl.ds(h0, chunk)]),
             (wg, wv.at[pl.ds(g0, ff)]), (wu, wv.at[pl.ds(g0 + ff, ff)]),
             (wd, wv.at[pl.ds(d_0, ff)]),
             (hid.at[pl.ds(chunk, rows - chunk)], wv.at[pl.ds(h0 + chunk, rows - chunk)])]
    head_rows = split(0, h0, 9)
    tail_rows = split(h0, vocab, 2)
    loads = [pltpu.make_async_copy(a, b, load_sem.at[i]) for i, (a, b) in enumerate(first)]
    loads += [pltpu.make_async_copy(wvt.at[pl.ds(a, n)], wv.at[pl.ds(a, n)], load_sem.at[len(first) + i])
              for i, (a, n) in enumerate(head_rows + tail_rows)]
    nf, nh = len(first), len(head_rows)
    for cp in loads[:nf]:
        cp.start()
    hcopy = [pltpu.make_async_copy(hid3.at[ch * group + mine], hs.at[ch], hs_sem.at[ch]) for ch in range(CHUNKS)]
    for cp in hcopy:
        cp.start()

    barrier = pltpu.get_barrier_semaphore()
    for k in range(1, group):
        pl.semaphore_signal(barrier, inc=1, device_id=other(k), device_id_type=MESH)

    def mlp(ch):
        gu = lax.dot_general(wv[pl.ds(g0, 2 * ff), :], wv[pl.ds(h0 + ch * chunk, chunk), :], NT,
                             preferred_element_type=F32)
        at = jax.nn.silu(gu[:ff]) * gu[ff:]
        act[...] = at.T.astype(BF16)
        step = 256
        for n in range(width // step):
            cols = pl.ds(n * step, step)
            part = jnp.dot(act[...], wv[pl.ds(d_0, ff), cols], preferred_element_type=F32)
            yp[ch, :, :, cols] = part.reshape(group, chunk // group, step).astype(BF16)

    def s0(ch):
        return remote(yp.at[ch, pl.ds((1 - core) * half, half)], d0.at[ch], s0_s.at[ch], s0_r.at[ch], partner)

    def s1(ch, d):
        to = lax.rem(f + d, n2)
        return remote(yp.at[ch, pl.ds(slab(to, 0), n2)], st1.at[ch, d - 1], s1_s.at[ch, d - 1],
                      s1_r.at[ch, d - 1], dev(to, s))

    def s2(ch, d):
        to = lax.rem(s + d, n2)
        return remote(yp.at[ch, slab(f, to)], st2.at[ch, d - 1], s2_s.at[ch, d - 1],
                      s2_r.at[ch, d - 1], dev(f, to))

    def add0(ch):
        s0(ch).wait_recv()

        def body(i, _):
            k = core * half + i
            yp[ch, k] = (yp[ch, k].astype(F32) + d0[ch, i].astype(F32)).astype(BF16)
            return 0
        lax.fori_loop(0, half, body, 0)

    def send1(ch):
        for d in (2, 1, 3):
            s1(ch, d).start()

    def add1(ch):
        for d in range(1, n2):
            s1(ch, d).wait_recv()

        def body(i, _):
            k = slab(f, i)
            acc = yp[ch, k].astype(F32)
            for d in range(n2 - 1):
                acc = acc + st1[ch, d, i].astype(F32)
            yp[ch, k] = acc.astype(BF16)
            return 0
        lax.fori_loop(0, n2, body, 0)

    def send2(ch):
        for d in (2, 1, 3):
            s2(ch, d).start()

    def norm(ch):
        hcopy[ch].wait()
        for d in range(1, n2):
            s2(ch, d).wait_recv()
        acc = yp[ch, mine].astype(F32)
        for d in range(n2 - 1):
            acc = acc + st2[ch, d].astype(F32)
        r = hs[ch].astype(F32) + acc.astype(BF16).astype(F32)
        inv = lax.rsqrt(jnp.mean(r * r, axis=-1, keepdims=True) + NORM_EPS)
        xf[ch, mine] = (gain[...] * r * inv).astype(BF16)

    def ga(ch, d):
        to = lax.rem(s + d, n2)
        ref = xf.at[ch, mine]
        return remote(ref, ref, ga_s.at[ch, d - 1], g_r.at[ch, mine], dev(f, to))

    def gb(ch, e, d):
        k = slab(f, lax.rem(s + n2 - e, n2))
        ref = xf.at[ch, k]
        return remote(ref, ref, gb_s.at[ch, e, d - 1], g_r.at[ch, k], dev(lax.rem(f + d, n2), s))

    def gc(ch, d, e):
        k = slab(lax.rem(f + n2 - d, n2), lax.rem(s + n2 - e, n2))
        ref = xf.at[ch, k]
        return remote(ref, ref, gc_s.at[ch, d, e], g_r.at[ch, k], partner)

    order = (0, 1, 3, 2)

    def gather_a(ch):
        for d in (2, 1, 3):
            ga(ch, d).start()
        for d in (2, 1, 3):
            gb(ch, 0, d).start()
        gc(ch, 0, 0).start()

    def got(ch, k):
        ref = xf.at[ch, k]
        remote(ref, ref, ga_s.at[ch, 0], g_r.at[ch, k], partner).wait_recv()

    def gather_b(ch):
        for e in order[1:]:
            got(ch, slab(f, lax.rem(s + n2 - e, n2)))
            for d in (2, 1, 3):
                gb(ch, e, d).start()
            gc(ch, 0, e).start()

    def gather_c(ch):
        for e in order:
            for d in order[1:]:
                got(ch, slab(lax.rem(f + n2 - d, n2), lax.rem(s + n2 - e, n2)))
                gc(ch, d, e).start()

    def gather_end(ch):
        for k in range(half):
            got(ch, (1 - core) * half + k)

        def body(j, _):
            v = xf[ch, pl.ds(2 * j, 2)].astype(F32).reshape(2 * (chunk // group), width)
            xm[ch, pl.ds(pl.multiple_of(j * 16, 16), 16), :] = v.astype(BF16)
            return 0
        lax.fori_loop(0, group // 2, body, 0)

    def head(ch, lo, hi, carry):
        cs = pl.ds(ch * chunk, chunk)
        inv_t = 1.0 / temp[0:1, cs]
        ids = tid[0:1, cs] - me * vocab

        def body(b, carry):
            m, sm, q, tg = carry
            rs = pl.ds(pl.multiple_of(b * block, 16), block)
            l = lax.dot_general(wv[rs, :], xm[ch], NT, preferred_element_type=F32) * inv_t
            lg[rs, cs] = l
            l3 = l.reshape(block // 8, 8, chunk)
            mn = jnp.maximum(m, jnp.max(l3, axis=0))
            a = jnp.exp(m - mn)
            e = jnp.exp(l3 - mn[None])
            row = (lax.broadcasted_iota(jnp.int32, l3.shape, 0) * 8
                   + lax.broadcasted_iota(jnp.int32, l3.shape, 1))
            hit = row == (ids - b * block)[None]
            return (mn, sm * a + jnp.sum(e, axis=0), q * a + jnp.sum(e * l3, axis=0),
                    tg + jnp.sum(jnp.where(hit, l3, 0.0), axis=0))
        return lax.fori_loop(lo, hi, body, carry)

    def start_carry():
        z = jnp.zeros((8, chunk), F32)
        return jnp.full((8, chunk), -3.4e38, F32), z, z, z

    def stat(ch, k):
        return remote(so.at[ch], sr.at[ch, me], so_s.at[ch, k - 1], so_r.at[ch, me], other(k))

    def stats_send(ch, carry):
        m8, s8, q8, t8 = carry
        m = jnp.max(m8, axis=0, keepdims=True)
        w = jnp.exp(m8 - m)
        so[ch, 0:1] = m
        so[ch, 1:2] = jnp.sum(s8 * w, axis=0, keepdims=True)
        so[ch, 2:3] = jnp.sum(q8 * w, axis=0, keepdims=True)
        so[ch, 3:4] = jnp.sum(t8, axis=0, keepdims=True)
        sr[ch, me] = so[ch]
        for k in range(1, group):
            stat(ch, k).start()

    def stats_end(ch):
        for k in range(1, group):
            i = lax.rem(me + k, group)
            remote(so.at[ch], sr.at[ch, i], so_s.at[ch, 0], so_r.at[ch, i], partner).wait_recv()
        m = sr[ch, :, 0, :]
        top = jnp.max(m, axis=0, keepdims=True)
        w = jnp.exp(m - top)
        total = jnp.sum(sr[ch, :, 1, :] * w, axis=0, keepdims=True)
        moment = jnp.sum(sr[ch, :, 2, :] * w, axis=0, keepdims=True)
        target = jnp.sum(sr[ch, :, 3, :], axis=0, keepdims=True)
        log_norm = top + jnp.log(total)
        cs = pl.ds(ch * chunk, chunk)
        stats[0:1, cs] = log_norm
        stats[1:2, cs] = log_norm - moment / total
        stats[2:3, cs] = target - log_norm

    for cp in loads[:nf - 1]:
        cp.wait()
    for cp in loads[nf:nf + nh]:
        cp.start()
    mlp(0)
    pl.semaphore_wait(barrier, group - 1)
    s0(0).start()
    loads[nf - 1].wait()
    mlp(1)
    s0(1).start()
    for cp in loads[nf + nh:]:
        cp.start()
    add0(0)
    send1(0)
    add0(1)
    add1(0)
    send2(0)
    send1(1)
    norm(0)
    gather_a(0)
    gather_b(0)
    gather_c(0)
    gather_end(0)
    add1(1)
    send2(1)
    for cp in loads[nf:]:
        cp.wait()
    carry = head(0, 0, 3, start_carry())
    norm(1)
    gather_a(1)
    carry = head(0, 3, 6, carry)
    gather_b(1)
    carry = head(0, 6, 9, carry)
    gather_c(1)
    carry = head(0, 9, BLOCKS, carry)
    stats_send(0, carry)
    gather_end(1)
    carry = head(1, 0, BLOCKS, start_carry())
    stats_send(1, carry)
    stats_end(0)
    stats_end(1)
    for ch in range(CHUNKS):
        s0(ch).wait_send()
        for d in range(1, n2):
            s1(ch, d).wait_send()
            s2(ch, d).wait_send()
            ga(ch, d).wait_send()
            for e in range(n2):
                gb(ch, e, d).wait_send()
        for d in range(n2):
            for e in range(n2):
                gc(ch, d, e).wait_send()
        for k in range(1, group):
            stat(ch, k).wait_send()


def final_kernel(lg, stats, out, buf, sem):
    vocab = lg.shape[0]
    step = buf.shape[1]
    steps, slots = vocab // step, buf.shape[0]

    def copy(i):
        return pltpu.make_async_copy(buf.at[i % slots], out.at[pl.ds(i * step, step)], sem.at[i % slots])

    for i in range(steps):
        if i >= slots:
            copy(i - slots).wait()
        buf[i % slots] = (lg[pl.ds(i * step, step), :] - stats[0:1, :]).astype(BF16)
        copy(i).start()
    for i in range(max(0, steps - slots), steps):
        copy(i).wait()


def solution(mesh):
    model_axes = ('tp2', 'tp')
    n2, n1 = mesh.shape['tp2'], mesh.shape['tp']
    group, nx = n2 * n1, n1 // CORES
    assert nx == n2

    def local_step(hidden, w_gate, w_up, w_down, norm_gain, w_vocab, temperature, target_ids):
        rows, width = hidden.shape
        ff, vocab = w_gate.shape[1], w_vocab.shape[1]
        chunk = rows // CHUNKS
        sl = chunk // group
        half = group // CORES
        hbm, vmem = pl.BlockSpec(memory_space=pl.ANY), pl.BlockSpec(memory_space=pltpu.VMEM)
        dma = pltpu.SemaphoreType.DMA
        c = CHUNKS
        lg, stats = pl.pallas_call(
            lambda *refs: main_kernel(n2, n1, *refs),
            out_shape=(pltpu.VMEM((vocab, rows), F32), pltpu.VMEM((3, rows), F32)),
            in_specs=[hbm] * 5 + [vmem, hbm, vmem, vmem],
            out_specs=(vmem, vmem),
            scratch_shapes=[
                pltpu.VMEM((vocab, width), BF16),
                pltpu.VMEM((c, group, sl, width), BF16),
                pltpu.VMEM((c, half, sl, width), BF16),
                pltpu.VMEM((c, n2 - 1, n2, sl, width), BF16),
                pltpu.VMEM((c, n2 - 1, sl, width), BF16),
                pltpu.VMEM((c, group, sl, width), BF16),
                pltpu.VMEM((c, chunk, width), BF16),
                pltpu.VMEM((c, sl, width), BF16),
                pltpu.VMEM((chunk, ff), BF16),
                pltpu.VMEM((c, 4, chunk), F32),
                pltpu.VMEM((c, group, 4, chunk), F32),
                dma((24,)), dma((c,)), dma((c,)), dma((c,)),
                dma((c, n2 - 1)), dma((c, n2 - 1)), dma((c, n2 - 1)), dma((c, n2 - 1)),
                dma((c, n2 - 1)), dma((c, n2, n2 - 1)), dma((c, n2, n2)), dma((c, group)),
                dma((c, group - 1)), dma((c, group)),
            ],
            name='mlp_head',
            cost_estimate=pl.CostEstimate(flops=2 * rows * width * (vocab + 3 * ff),
                                          bytes_accessed=2 * width * vocab, transcendentals=rows * vocab),
            compiler_params=pltpu.CompilerParams(collective_id=0, has_side_effects=True,
                                                 vmem_limit_bytes=47 * 1024 * 1024),
        )(hidden, hidden.reshape(rows // sl, sl, width), w_gate.T, w_up.T, w_down, norm_gain[None, :],
          w_vocab.T, temperature[None, :], target_ids[None, :])
        out = pl.pallas_call(
            final_kernel,
            out_shape=jax.ShapeDtypeStruct((vocab, rows), BF16),
            in_specs=[vmem, vmem],
            out_specs=hbm,
            scratch_shapes=[pltpu.VMEM((4, vocab // 20, rows), BF16), dma((4,))],
            name='logprobs',
            compiler_params=pltpu.CompilerParams(vmem_limit_bytes=16 * 1024 * 1024),
        )(lg, stats)
        return stats[0], stats[1], stats[2], out.T

    return jax.shard_map(
        local_step, mesh=mesh,
        in_specs=(P('dp', None), P(None, model_axes), P(None, model_axes), P(model_axes, None),
                  P(None), P(None, model_axes), P('dp'), P('dp')),
        out_specs=(P('dp'), P('dp'), P('dp'), P('dp', model_axes)),
        check_vma=False)
```

```python
import functools

import jax
import jax.numpy as jnp
from jax import lax
from jax.experimental import pallas as pl
from jax.experimental.pallas import tpu as pltpu
from jax.sharding import PartitionSpec as P

NORM_EPS = 1e-6
CORES = 2
HALVES = 2
BLOCKS = 20
UNROLL = 2
UNIT = 32
MESH = pl.DeviceIdType.MESH
NT = (((1,), (1,)), ((), ()))
F32, BF16 = jnp.float32, jnp.bfloat16


def split(start, stop, pieces):
    step = -(-(stop - start) // pieces)
    step = -(-step // 16) * 16
    return [(i, min(step, stop - i)) for i in range(start, stop, step)]


def main_kernel(n2, n1, hid, hid3, wg, wu, wd, gain, wvt, temp, tid, lg, stats,
                wv, yp, d0, fw, nb, st2, xf, hs, act, gain_v, temp_v, tid_v, so, pair_st, chip_st, sr, done,
                load_sem, hs_sem, small_sem, s0_s, s0_r, fw_s, fw_r, nb_s, nb_r, s2_s, s2_r,
                ga_s, gb_s, gf_s, gc_s, g_r, sw_s, sw_r, so_s, so_r):
    group = n1 * n2
    half = group // CORES
    rows, width = hid.shape
    ff = wg.shape[0]
    vocab = wvt.shape[0]
    chunk = rows // HALVES
    block = vocab // BLOCKS

    y = lax.axis_index('tp2')
    t = lax.axis_index('tp')
    core = lax.rem(t, CORES)
    x = lax.div(t, CORES)
    me = y * n1 + t
    f = y + core * (x - y)
    s = x + core * (y - x)
    mine = core * half + f * n2 + s

    def dev(a, b):
        return {'tp2': a + core * (b - a), 'tp': CORES * (b + core * (a - b)) + core}

    partner = {'tp2': y, 'tp': CORES * x + (1 - core)}

    def slab(a, b):
        return core * half + a * n2 + b

    def remote(src, dst, ssem, rsem, to):
        return pltpu.make_async_remote_copy(src_ref=src, dst_ref=dst, send_sem=ssem, recv_sem=rsem,
                                            device_id=to, device_id_type=MESH)

    right, left, far = (lax.rem(f + i, n2) for i in (1, n2 - 1, 2))
    peers = [dev(right, s), dev(left, s), partner] + [dev(f, lax.rem(s + d, n2)) for d in range(1, n2)]
    barrier = pltpu.get_barrier_semaphore()
    for p in peers:
        pl.semaphore_signal(barrier, inc=1, device_id=p, device_id_type=MESH)

    h0 = vocab - 3 * ff - rows
    g0, d_0 = h0 + rows, h0 + rows + 2 * ff
    theirs = pl.multiple_of((1 - core) * chunk, chunk)
    own = pl.multiple_of(core * chunk, chunk)
    first = [(hid.at[pl.ds(theirs, chunk)], wv.at[pl.ds(h0 + theirs, chunk)]),
             (wg, wv.at[pl.ds(g0, ff)]), (wu, wv.at[pl.ds(g0 + ff, ff)]),
             (wd, wv.at[pl.ds(d_0, ff)]),
             (hid.at[pl.ds(own, chunk)], wv.at[pl.ds(h0 + own, chunk)])]
    head_rows = split(0, h0, 9)
    tail_rows = split(h0, vocab, 2)
    loads = [pltpu.make_async_copy(a, b, load_sem.at[i]) for i, (a, b) in enumerate(first)]
    loads += [pltpu.make_async_copy(wvt.at[pl.ds(a, n)], wv.at[pl.ds(a, n)], load_sem.at[len(first) + i])
              for i, (a, n) in enumerate(head_rows + tail_rows)]
    nf, nh = len(first), len(head_rows)
    for cp in loads[:nf]:
        cp.start()
    hcopy = [pltpu.make_async_copy(hid3.at[mine], hs, hs_sem)]
    small = [pltpu.make_async_copy(a, b, small_sem.at[i])
             for i, (a, b) in enumerate(((gain, gain_v), (temp, temp_v), (tid, tid_v)))]
    for cp in hcopy + small:
        cp.start()

    def gate_up(ch):
        gu = lax.dot_general(wv[pl.ds(g0, 2 * ff), :], wv[pl.ds(pl.multiple_of(h0 + ch * chunk, 16), chunk), :], NT,
                             preferred_element_type=F32)
        at = jax.nn.silu(gu[:ff]) * gu[ff:]
        act[...] = at.T.astype(BF16)

    def down(ch):
        step = 256
        for n in range(width // step):
            cols = pl.ds(n * step, step)
            part = jnp.dot(act[...], wv[pl.ds(d_0, ff), cols], preferred_element_type=F32)
            yp[pl.ds(ch * half, half), :, cols] = part.reshape(half, rows // group, step).astype(BF16)

    def s0():
        return remote(yp.at[pl.ds((1 - core) * half, half)], d0, s0_s, s0_r, partner)

    LATE = ((2, 1), (3, 0))

    def at_s(d):
        return lax.rem(s + d, n2)

    def send_fw(i, j):
        return remote(yp.at[slab(far, at_s(LATE[i][j]))], fw.at[i, j], fw_s.at[i, j],
                      fw_r.at[i, j], dev((right, left)[i], s))

    def send_nb(i, d):
        to = (right, left)[i]
        return remote(yp.at[slab(to, at_s(d))], nb.at[i, d], nb_s.at[i, d],
                      nb_r.at[i, d], dev(to, s))

    def s2(d):
        to = lax.rem(s + d, n2)
        return remote(yp.at[slab(f, to)], st2.at[d - 1], s2_s.at[d - 1],
                      s2_r.at[d - 1], dev(f, to))

    def add0():
        s0().wait_recv()

        def body(i, _):
            k = core * half + i
            yp[k] = (yp[k].astype(F32) + d0[i].astype(F32)).astype(BF16)
            return 0
        lax.fori_loop(0, half, body, 0)

    def send1():
        for j in (0, 1):
            for i in (0, 1):
                send_fw(i, j).start()
        for j in (0, 1):
            for i in (0, 1):
                send_nb(i, LATE[1 - i][j]).start()

    def pass1():
        for j in (0, 1):
            for i in (0, 1):
                d = LATE[i][j]
                send_fw(i, j).wait_recv()
                k = slab((right, left)[i], at_s(d))
                yp[k] = (yp[k].astype(F32) + fw[i, j].astype(F32)).astype(BF16)
                send_nb(i, d).start()

    def add1():
        for d in (2, 3, 1, 0):
            for i in (0, 1):
                send_nb(i, d).wait_recv()
            k = slab(f, at_s(d))
            yp[k] = (yp[k].astype(F32) + nb[0, d].astype(F32) + nb[1, d].astype(F32)).astype(BF16)
            if d:
                s2(d).start()

    def norm():
        for d in range(1, n2):
            s2(d).wait_recv()
        acc = yp[mine].astype(F32)
        for d in range(n2 - 1):
            acc = acc + st2[d].astype(F32)
        r = hs[...].astype(F32) + acc.astype(BF16).astype(F32)
        inv = lax.rsqrt(jnp.mean(r * r, axis=-1, keepdims=True) + NORM_EPS)
        xf[mine] = (gain_v[...].reshape(1, width) * r * inv).astype(BF16)

    def ga(d):
        ref = xf.at[mine]
        return remote(ref, ref, ga_s.at[d - 1], g_r.at[mine], dev(f, at_s(d)))

    def back(a, e):
        return slab(a, at_s(n2 - e))

    def gb(i, e):
        k = back(f, e)
        ref = xf.at[k]
        return remote(ref, ref, gb_s.at[i, e], g_r.at[k], dev((right, left)[i], s))

    PASS = ((0, 1), (3, 2))

    def gf(i, j):
        k = back((left, right)[i], PASS[i][j])
        ref = xf.at[k]
        return remote(ref, ref, gf_s.at[i, j], g_r.at[k], dev((right, left)[i], s))

    def gc(d, e):
        k = back(lax.rem(f + d, n2), e)
        ref = xf.at[k]
        return remote(ref, ref, gc_s.at[d, e], g_r.at[k], partner)

    def got(k):
        ref = xf.at[k]
        remote(ref, ref, ga_s.at[0], g_r.at[k], partner).wait_recv()

    def out_own(e):
        if e:
            got(back(f, e))
        for i in (0, 1):
            gb(i, e).start()
        gc(0, e).start()

    def from_side(e):
        for i in ((0, 1) if e in PASS[0] else (1, 0)):
            got(back((left, right)[i], e))
            if e in PASS[i]:
                gf(i, PASS[i].index(e)).start()
            gc((n2 - 1, 1)[i], e).start()

    def from_far(e):
        got(back(far, e))
        gc(2, e).start()

    def gather(part):
        if part == 0:
            for d in (2, 1, 3):
                ga(d).start()
            out_own(0)
        elif part == 1:
            out_own(1)
            out_own(3)
        elif part == 2:
            from_side(0)
            out_own(2)
        elif part == 3:
            from_side(1)
            from_side(3)
        elif part == 4:
            from_far(0)
            from_side(2)
        else:
            for e in (1, 3, 2):
                from_far(e)

    def gather_end():
        for k in range(half):
            got((1 - core) * half + k)

    def head():
        inv_t = 1.0 / temp_v[...]
        lanes = lax.broadcasted_iota(jnp.int32, (8, rows), 0)
        ids = tid_v[...] - me * vocab - lanes

        def products(i):
            for u in range(UNROLL):
                rs = pl.ds(pl.multiple_of((i * UNROLL + u) * block, 16), block)
                l = lax.dot_general(wv[rs, :], xf[...].reshape(rows, width), NT, preferred_element_type=F32)
                lg[rs, :] = l * inv_t

        def update(i, carry):
            m, total, moment, target = carry
            for u in range(UNROLL):
                base = (i * UNROLL + u) * block
                here = ids - base
                for g in range(0, block, UNIT):
                    n = min(UNIT, block - g)
                    l = lg[pl.ds(pl.multiple_of(base + g, 8), n), :]
                    parts = [l[j:j + 8] for j in range(0, n, 8)]
                    tops = parts
                    while len(tops) > 1:
                        tops = [jnp.maximum(*tops[j:j + 2]) if j + 1 < len(tops) else tops[j]
                                for j in range(0, len(tops), 2)]
                    top = jnp.maximum(m, tops[0])
                    scale = jnp.exp(m - top)
                    total, moment, m = total * scale, moment * scale, top
                    for j, p in enumerate(parts):
                        e = jnp.exp(p - top)
                        total, moment = total + e, moment + e * p
                        target = jnp.where(here == g + 8 * j, p, target)
            return m, total, moment, target

        def body(i, carry):
            carry = update(i - 1, carry)
            products(i)
            return carry

        z = jnp.zeros((8, rows), F32)
        products(0)
        steps = BLOCKS // UNROLL
        carry = lax.fori_loop(1, steps, body, (jnp.full((8, rows), -3.4e38, F32), z, z, z))
        return update(steps - 1, carry)

    chips = group // CORES
    chip = y * (n1 // CORES) + x

    def swap(src, dst, k):
        return remote(src, dst, sw_s.at[k], sw_r.at[k], partner)

    def stat(k):
        i = lax.rem(chip + k, chips)
        to = {'tp2': lax.div(i, n1 // CORES), 'tp': CORES * lax.rem(i, n1 // CORES) + core}
        return remote(chip_st, sr.at[chip], so_s.at[k - 1], so_r.at[chip], to)

    def statistics(carry):
        m8, s8, q8, t8 = carry
        m = jnp.max(m8, axis=0, keepdims=True)
        w = jnp.exp(m8 - m)
        rows4 = [m, jnp.sum(s8 * w, axis=0, keepdims=True), jnp.sum(q8 * w, axis=0, keepdims=True),
                 jnp.sum(t8, axis=0, keepdims=True)]
        for j in range(4):
            for h in range(HALVES):
                so[h, j:j + 1] = rows4[j][:, h * chunk:(h + 1) * chunk]
        first = swap(so.at[1 - core], pair_st, 0)
        first.start()
        first.wait_recv()
        a, b = so[core], pair_st[...]
        m = jnp.maximum(a[0:1], b[0:1])
        wa, wb = jnp.exp(a[0:1] - m), jnp.exp(b[0:1] - m)
        chip_st[0:1] = m
        chip_st[1:3] = a[1:3] * wa + b[1:3] * wb
        chip_st[3:4] = a[3:4] + b[3:4]
        for k in range(1, chips):
            stat(k).start()
        sr[chip] = chip_st[...]
        for k in range(1, chips):
            i = lax.rem(chip + k, chips)
            remote(chip_st, sr.at[i], so_s.at[0], so_r.at[i], partner).wait_recv()
        m = sr[:, 0, :]
        top = jnp.max(m, axis=0, keepdims=True)
        w = jnp.exp(m - top)
        total = jnp.sum(sr[:, 1, :] * w, axis=0, keepdims=True)
        moment = jnp.sum(sr[:, 2, :] * w, axis=0, keepdims=True)
        log_norm = top + jnp.log(total)
        done[core, 0:1] = log_norm
        done[core, 1:2] = log_norm - moment / total
        done[core, 2:3] = jnp.sum(sr[:, 3, :], axis=0, keepdims=True) - log_norm
        second = swap(done.at[core], done.at[core], 1)
        second.start()
        swap(done.at[1 - core], done.at[1 - core], 1).wait_recv()
        for h in range(HALVES):
            stats[:, h * chunk:(h + 1) * chunk] = done[h, 0:3]
        first.wait_send()
        second.wait_send()
        for k in range(1, chips):
            stat(k).wait_send()

    for cp in loads[:nf - 1]:
        cp.wait()
    for cp in loads[nf:nf + nh]:
        cp.start()
    gate_up(1 - core)
    down(1 - core)
    pl.semaphore_wait(barrier, len(peers))
    s0().start()
    loads[nf - 1].wait()
    gate_up(core)
    down(core)
    for cp in loads[nf + nh:]:
        cp.start()
    add0()
    send1()
    pass1()
    for cp in hcopy + small:
        cp.wait()
    add1()
    norm()
    for part in range(6):
        gather(part)
    gather_end()
    for cp in loads[nf:]:
        cp.wait()
    carry = head()
    statistics(carry)
    s0().wait_send()
    for i in (0, 1):
        for j in (0, 1):
            send_fw(i, j).wait_send()
            gf(i, j).wait_send()
        for d in range(n2):
            send_nb(i, d).wait_send()
            gb(i, d).wait_send()
    for d in range(1, n2):
        s2(d).wait_send()
        ga(d).wait_send()
    for d in range(n2):
        for e in range(n2):
            gc(d, e).wait_send()


def final_kernel(lg, stats, out, *rest):
    outs, rows, (buf, sem, row_sem) = rest[:3], rest[3:6], rest[6:]
    vocab = lg.shape[0]
    step = buf.shape[1]
    steps, slots = vocab // step, buf.shape[0]

    def copy(i):
        return pltpu.make_async_copy(buf.at[i % slots], out.at[pl.ds(i * step, step)], sem.at[i % slots])

    for i in range(steps):
        if i >= slots:
            copy(i - slots).wait()
        buf[i % slots] = (lg[pl.ds(i * step, step), :] - stats[0:1, :]).astype(BF16)
        copy(i).start()
        if i == 0:
            small = [pltpu.make_async_copy(rows[j], outs[j], row_sem.at[j]) for j in range(3)]
            for j in range(3):
                rows[j][...] = stats[j, :]
            for cp in small:
                cp.start()
    for cp in small:
        cp.wait()
    for i in range(max(0, steps - slots), steps):
        copy(i).wait()


def solution(mesh):
    model_axes = ('tp2', 'tp')
    n2, n1 = mesh.shape['tp2'], mesh.shape['tp']
    group, nx = n2 * n1, n1 // CORES
    assert nx == n2

    def local_step(hidden, w_gate, w_up, w_down, norm_gain, w_vocab, temperature, target_ids):
        rows, width = hidden.shape
        ff, vocab = w_gate.shape[1], w_vocab.shape[1]
        sl = rows // group
        half = group // CORES
        hbm, vmem = pl.BlockSpec(memory_space=pl.ANY), pl.BlockSpec(memory_space=pltpu.VMEM)
        dma = pltpu.SemaphoreType.DMA
        lg, stats = pl.pallas_call(
            lambda *refs: main_kernel(n2, n1, *refs),
            out_shape=(pltpu.VMEM((vocab, rows), F32), pltpu.VMEM((3, rows), F32)),
            in_specs=[hbm] * 9,
            out_specs=(vmem, vmem),
            scratch_shapes=[
                pltpu.VMEM((vocab, width), BF16),
                pltpu.VMEM((group, sl, width), BF16),
                pltpu.VMEM((half, sl, width), BF16),
                pltpu.VMEM((2, 2, sl, width), BF16),
                pltpu.VMEM((2, n2, sl, width), BF16),
                pltpu.VMEM((n2 - 1, sl, width), BF16),
                pltpu.VMEM((group, sl, width), BF16),
                pltpu.VMEM((sl, width), BF16),
                pltpu.VMEM((rows // HALVES, ff), BF16),
                pltpu.VMEM((width,), F32),
                pltpu.VMEM((1, rows), F32),
                pltpu.VMEM((1, rows), jnp.int32),
                pltpu.VMEM((HALVES, 4, rows // HALVES), F32),
                pltpu.VMEM((4, rows // HALVES), F32),
                pltpu.VMEM((4, rows // HALVES), F32),
                pltpu.VMEM((half, 4, rows // HALVES), F32),
                pltpu.VMEM((HALVES, 4, rows // HALVES), F32),
                dma((24,)), dma, dma((3,)), dma, dma,
                dma((2, 2)), dma((2, 2)), dma((2, n2)), dma((2, n2)), dma((n2 - 1,)), dma((n2 - 1,)),
                dma((n2 - 1,)), dma((2, n2)), dma((2, 2)), dma((n2, n2)), dma((group,)),
                dma((2,)), dma((2,)), dma((half - 1,)), dma((half,)),
            ],
            name='mlp_head',
            cost_estimate=pl.CostEstimate(flops=2 * rows * width * (vocab + 3 * ff),
                                          bytes_accessed=2 * width * vocab, transcendentals=rows * vocab),
            compiler_params=pltpu.CompilerParams(collective_id=0, has_side_effects=True,
                                                 vmem_limit_bytes=47 * 1024 * 1024),
        )(hidden, hidden.reshape(group, sl, width), w_gate.T, w_up.T, w_down, norm_gain,
          w_vocab.T, temperature[None, :], target_ids[None, :])
        row = jax.ShapeDtypeStruct((rows,), F32)
        out, *small = pl.pallas_call(
            final_kernel,
            out_shape=(jax.ShapeDtypeStruct((vocab, rows), BF16), row, row, row),
            in_specs=[vmem, vmem],
            out_specs=(hbm,) * 4,
            scratch_shapes=[pltpu.VMEM((rows,), F32)] * 3 + [pltpu.VMEM((4, vocab // 10, rows), BF16), dma((4,)), dma((3,))],
            name='logprobs',
            compiler_params=pltpu.CompilerParams(vmem_limit_bytes=16 * 1024 * 1024),
        )(lg, stats)
        return *small, out.T

    return jax.shard_map(
        local_step, mesh=mesh,
        in_specs=(P('dp', None), P(None, model_axes), P(None, model_axes), P(model_axes, None),
                  P(None), P(None, model_axes), P('dp'), P('dp')),
        out_specs=(P('dp'), P('dp'), P('dp'), P('dp', model_axes)),
        check_vma=False)
```

```python
import functools

import jax
import jax.numpy as jnp
from jax import lax
from jax.experimental import pallas as pl
from jax.experimental.pallas import tpu as pltpu
from jax.sharding import PartitionSpec as P

NORM_EPS = 1e-6
CORES = 2
HALVES = 2
CHUNKS = 2
BLOCKS = 20
UNROLL = 2
UNIT = 32
MESH = pl.DeviceIdType.MESH
NT = (((1,), (1,)), ((), ()))
F32, BF16 = jnp.float32, jnp.bfloat16


def split(start, stop, pieces):
    step = -(-(stop - start) // pieces)
    step = -(-step // 16) * 16
    return [(i, min(step, stop - i)) for i in range(start, stop, step)]


def main_kernel(n2, n1, hid, hid3, wg, wu, wd, gain, wvt, temp, tid, lg, stats,
                wv, yp, d0, fw, nb, st2, xf, xm, hs, act, gain_v, temp_v, tid_v, so, pair_st, chip_st, sr, done,
                load_sem, hs_sem, small_sem, s0_s, s0_r, fw_s, fw_r, nb_s, nb_r, s2_s, s2_r,
                ga_s, gb_s, gf_s, gc_s, g_r, sw_s, sw_r, so_s, so_r):
    group = n1 * n2
    half = group // CORES
    rows, width = hid.shape
    ff = wg.shape[0]
    vocab = wvt.shape[0]
    chunk = rows // CHUNKS
    block = vocab // BLOCKS

    y = lax.axis_index('tp2')
    t = lax.axis_index('tp')
    core = lax.rem(t, CORES)
    x = lax.div(t, CORES)
    me = y * n1 + t
    f = y + core * (x - y)
    s = x + core * (y - x)
    mine = core * half + f * n2 + s

    def dev(a, b):
        return {'tp2': a + core * (b - a), 'tp': CORES * (b + core * (a - b)) + core}

    partner = {'tp2': y, 'tp': CORES * x + (1 - core)}

    def slab(a, b):
        return core * half + a * n2 + b

    def remote(src, dst, ssem, rsem, to):
        return pltpu.make_async_remote_copy(src_ref=src, dst_ref=dst, send_sem=ssem, recv_sem=rsem,
                                            device_id=to, device_id_type=MESH)

    right, left, far = (lax.rem(f + i, n2) for i in (1, n2 - 1, 2))
    peers = [dev(right, s), dev(left, s), partner] + [dev(f, lax.rem(s + d, n2)) for d in range(1, n2)]
    barrier = pltpu.get_barrier_semaphore()
    for p in peers:
        pl.semaphore_signal(barrier, inc=1, device_id=p, device_id_type=MESH)

    h0 = vocab - 3 * ff - rows
    g0, d_0 = h0 + rows, h0 + rows + 2 * ff
    quarter = chunk // CORES
    need = [1 - core, core]

    def rows_of(j):
        return [(hid.at[pl.ds(pl.multiple_of(ch * chunk + need[j] * quarter, quarter), quarter)],
                 wv.at[pl.ds(h0 + j * chunk + ch * quarter, quarter)]) for ch in range(CHUNKS)]

    first = [(wg, wv.at[pl.ds(g0, ff)]), (wu, wv.at[pl.ds(g0 + ff, ff)])] + rows_of(0) + rows_of(1)
    first += [(wd, wv.at[pl.ds(d_0, ff)])]
    head_rows = split(0, h0, 9)
    tail_rows = split(h0, vocab, 2)
    loads = [pltpu.make_async_copy(a, b, load_sem.at[i]) for i, (a, b) in enumerate(first)]
    loads += [pltpu.make_async_copy(wvt.at[pl.ds(a, n)], wv.at[pl.ds(a, n)], load_sem.at[len(first) + i])
              for i, (a, n) in enumerate(head_rows + tail_rows)]
    nf, nh = len(first), len(head_rows)
    for cp in loads[:nf]:
        cp.start()
    hcopy = [pltpu.make_async_copy(hid3.at[ch * group + mine], hs.at[ch], hs_sem.at[ch]) for ch in range(CHUNKS)]
    small = [pltpu.make_async_copy(a, b, small_sem.at[i])
             for i, (a, b) in enumerate(((gain, gain_v), (temp, temp_v), (tid, tid_v)))]
    for cp in hcopy + small:
        cp.start()

    def gate_up():
        gu = lax.dot_general(wv[pl.ds(g0, 2 * ff), :], wv[pl.ds(h0, rows), :], NT, preferred_element_type=F32)
        at = jax.nn.silu(gu[:ff]) * gu[ff:]
        act[...] = at.T.astype(BF16)

    def down(j):
        step = 256
        for n in range(width // step):
            cols = pl.ds(n * step, step)
            part = jnp.dot(act[pl.ds(j * chunk, chunk), :], wv[pl.ds(d_0, ff), cols], preferred_element_type=F32)
            yp[:, pl.ds(need[j] * half, half), :, cols] = part.reshape(
                CHUNKS, half, chunk // group, step).astype(BF16)

    def s0(ch):
        return remote(yp.at[ch, pl.ds((1 - core) * half, half)], d0.at[ch], s0_s.at[ch], s0_r.at[ch], partner)

    LATE = ((2, 1), (3, 0))

    def at_s(d):
        return lax.rem(s + d, n2)

    def send_fw(ch, i, j):
        return remote(yp.at[ch, slab(far, at_s(LATE[i][j]))], fw.at[ch, i, j], fw_s.at[ch, i, j],
                      fw_r.at[ch, i, j], dev((right, left)[i], s))

    def send_nb(ch, i, d):
        to = (right, left)[i]
        return remote(yp.at[ch, slab(to, at_s(d))], nb.at[ch, i, d], nb_s.at[ch, i, d],
                      nb_r.at[ch, i, d], dev(to, s))

    def s2(ch, d):
        to = lax.rem(s + d, n2)
        return remote(yp.at[ch, slab(f, to)], st2.at[ch, d - 1], s2_s.at[ch, d - 1],
                      s2_r.at[ch, d - 1], dev(f, to))

    def add0(ch):
        s0(ch).wait_recv()

        def body(i, _):
            k = core * half + i
            yp[ch, k] = (yp[ch, k].astype(F32) + d0[ch, i].astype(F32)).astype(BF16)
            return 0
        lax.fori_loop(0, half, body, 0)

    def send1(ch):
        for j in (0, 1):
            for i in (0, 1):
                send_fw(ch, i, j).start()

    def send1b(ch):
        for j in (0, 1):
            for i in (0, 1):
                send_nb(ch, i, LATE[1 - i][j]).start()

    def pass1(ch):
        for j in (0, 1):
            for i in (0, 1):
                d = LATE[i][j]
                send_fw(ch, i, j).wait_recv()
                k = slab((right, left)[i], at_s(d))
                yp[ch, k] = (yp[ch, k].astype(F32) + fw[ch, i, j].astype(F32)).astype(BF16)
                send_nb(ch, i, d).start()

    def add1(ch):
        for d in (2, 3, 1, 0):
            for i in (0, 1):
                send_nb(ch, i, d).wait_recv()
            k = slab(f, at_s(d))
            yp[ch, k] = (yp[ch, k].astype(F32) + nb[ch, 0, d].astype(F32) + nb[ch, 1, d].astype(F32)).astype(BF16)
            if d:
                s2(ch, d).start()

    def norm(ch):
        for d in range(1, n2):
            s2(ch, d).wait_recv()
        acc = yp[ch, mine].astype(F32)
        for d in range(n2 - 1):
            acc = acc + st2[ch, d].astype(F32)
        r = hs[ch].astype(F32) + acc.astype(BF16).astype(F32)
        inv = lax.rsqrt(jnp.mean(r * r, axis=-1, keepdims=True) + NORM_EPS)
        xf[ch, mine] = (gain_v[...].reshape(1, width) * r * inv).astype(BF16)

    def ga(ch, d):
        ref = xf.at[ch, mine]
        return remote(ref, ref, ga_s.at[ch, d - 1], g_r.at[ch, mine], dev(f, at_s(d)))

    def back(a, e):
        return slab(a, at_s(n2 - e))

    def gb(ch, i, e):
        k = back(f, e)
        ref = xf.at[ch, k]
        return remote(ref, ref, gb_s.at[ch, i, e], g_r.at[ch, k], dev((right, left)[i], s))

    PASS = ((0, 1), (3, 2))

    def gf(ch, i, j):
        k = back((left, right)[i], PASS[i][j])
        ref = xf.at[ch, k]
        return remote(ref, ref, gf_s.at[ch, i, j], g_r.at[ch, k], dev((right, left)[i], s))

    def gc(ch, d, e):
        k = back(lax.rem(f + d, n2), e)
        ref = xf.at[ch, k]
        return remote(ref, ref, gc_s.at[ch, d, e], g_r.at[ch, k], partner)

    def got(ch, k):
        ref = xf.at[ch, k]
        remote(ref, ref, ga_s.at[ch, 0], g_r.at[ch, k], partner).wait_recv()

    def out_own(ch, e):
        if e:
            got(ch, back(f, e))
        for i in (0, 1):
            gb(ch, i, e).start()
        gc(ch, 0, e).start()

    def from_side(ch, e):
        for i in ((0, 1) if e in PASS[0] else (1, 0)):
            got(ch, back((left, right)[i], e))
            if e in PASS[i]:
                gf(ch, i, PASS[i].index(e)).start()
            gc(ch, (n2 - 1, 1)[i], e).start()

    def from_far(ch, e):
        got(ch, back(far, e))
        gc(ch, 2, e).start()

    def gather(ch, part):
        if part == 0:
            for d in (2, 1, 3):
                ga(ch, d).start()
            out_own(ch, 0)
        elif part == 1:
            out_own(ch, 1)
            out_own(ch, 3)
        elif part == 2:
            from_side(ch, 0)
            out_own(ch, 2)
        elif part == 3:
            from_side(ch, 1)
            from_side(ch, 3)
        elif part == 4:
            from_far(ch, 0)
            from_side(ch, 2)
        else:
            for e in (1, 3, 2):
                from_far(ch, e)

    def gather_end(ch):
        for k in range(half):
            got(ch, (1 - core) * half + k)

        def body(j, _):
            v = xf[ch, pl.ds(2 * j, 2)].astype(F32).reshape(2 * (chunk // group), width)
            xm[pl.ds(pl.multiple_of(ch * chunk + j * 16, 16), 16), :] = v.astype(BF16)
            return 0
        lax.fori_loop(0, group // 2, body, 0)

    def head():
        inv_t = 1.0 / temp_v[...]
        lanes = lax.broadcasted_iota(jnp.int32, (8, rows), 0)
        ids = tid_v[...] - me * vocab - lanes

        def products(i):
            for u in range(UNROLL):
                rs = pl.ds(pl.multiple_of((i * UNROLL + u) * block, 16), block)
                l = lax.dot_general(wv[rs, :], xm[...], NT, preferred_element_type=F32)
                lg[rs, :] = l * inv_t

        def update(i, carry):
            m, total, moment, target = carry
            for u in range(UNROLL):
                base = (i * UNROLL + u) * block
                here = ids - base
                for g in range(0, block, UNIT):
                    n = min(UNIT, block - g)
                    l = lg[pl.ds(pl.multiple_of(base + g, 8), n), :]
                    parts = [l[j:j + 8] for j in range(0, n, 8)]
                    tops = parts
                    while len(tops) > 1:
                        tops = [jnp.maximum(*tops[j:j + 2]) if j + 1 < len(tops) else tops[j]
                                for j in range(0, len(tops), 2)]
                    top = jnp.maximum(m, tops[0])
                    scale = jnp.exp(m - top)
                    total, moment, m = total * scale, moment * scale, top
                    for j, p in enumerate(parts):
                        e = jnp.exp(p - top)
                        total, moment = total + e, moment + e * p
                        target = jnp.where(here == g + 8 * j, p, target)
            return m, total, moment, target

        def body(i, carry):
            carry = update(i - 1, carry)
            products(i)
            return carry

        z = jnp.zeros((8, rows), F32)
        products(0)
        steps = BLOCKS // UNROLL
        carry = lax.fori_loop(1, steps, body, (jnp.full((8, rows), -3.4e38, F32), z, z, z))
        return update(steps - 1, carry)

    chips = group // CORES
    chip = y * (n1 // CORES) + x

    def swap(src, dst, k):
        return remote(src, dst, sw_s.at[k], sw_r.at[k], partner)

    def stat(k):
        i = lax.rem(chip + k, chips)
        to = {'tp2': lax.div(i, n1 // CORES), 'tp': CORES * lax.rem(i, n1 // CORES) + core}
        return remote(chip_st, sr.at[chip], so_s.at[k - 1], so_r.at[chip], to)

    def statistics(carry):
        m8, s8, q8, t8 = carry
        m = jnp.max(m8, axis=0, keepdims=True)
        w = jnp.exp(m8 - m)
        rows4 = [m, jnp.sum(s8 * w, axis=0, keepdims=True), jnp.sum(q8 * w, axis=0, keepdims=True),
                 jnp.sum(t8, axis=0, keepdims=True)]
        for j in range(4):
            for h in range(HALVES):
                so[h, j:j + 1] = rows4[j][:, h * chunk:(h + 1) * chunk]
        first = swap(so.at[1 - core], pair_st, 0)
        first.start()
        first.wait_recv()
        a, b = so[core], pair_st[...]
        m = jnp.maximum(a[0:1], b[0:1])
        wa, wb = jnp.exp(a[0:1] - m), jnp.exp(b[0:1] - m)
        chip_st[0:1] = m
        chip_st[1:3] = a[1:3] * wa + b[1:3] * wb
        chip_st[3:4] = a[3:4] + b[3:4]
        for k in range(1, chips):
            stat(k).start()
        sr[chip] = chip_st[...]
        for k in range(1, chips):
            i = lax.rem(chip + k, chips)
            remote(chip_st, sr.at[i], so_s.at[0], so_r.at[i], partner).wait_recv()
        m = sr[:, 0, :]
        top = jnp.max(m, axis=0, keepdims=True)
        w = jnp.exp(m - top)
        total = jnp.sum(sr[:, 1, :] * w, axis=0, keepdims=True)
        moment = jnp.sum(sr[:, 2, :] * w, axis=0, keepdims=True)
        log_norm = top + jnp.log(total)
        done[core, 0:1] = log_norm
        done[core, 1:2] = log_norm - moment / total
        done[core, 2:3] = jnp.sum(sr[:, 3, :], axis=0, keepdims=True) - log_norm
        second = swap(done.at[core], done.at[core], 1)
        second.start()
        swap(done.at[1 - core], done.at[1 - core], 1).wait_recv()
        for h in range(HALVES):
            stats[:, h * chunk:(h + 1) * chunk] = done[h, 0:3]
        first.wait_send()
        second.wait_send()
        for k in range(1, chips):
            stat(k).wait_send()

    for cp in loads[:nf - 1]:
        cp.wait()
    gate_up()
    loads[nf - 1].wait()
    for cp in loads[nf:nf + nh]:
        cp.start()
    down(0)
    pl.semaphore_wait(barrier, len(peers))
    s0(0).start()
    s0(1).start()
    down(1)
    for cp in loads[nf + nh:]:
        cp.start()
    add0(0)
    send1(0)
    add0(1)
    send1(1)
    send1b(0)
    send1b(1)
    pass1(0)
    pass1(1)
    for cp in hcopy + small:
        cp.wait()
    add1(0)
    add1(1)
    norm(0)
    gather(0, 0)
    norm(1)
    gather(1, 0)
    gather(0, 1)
    gather(1, 1)
    gather(0, 2)
    gather(1, 2)
    gather(0, 3)
    gather(1, 3)
    gather(0, 4)
    gather(1, 4)
    gather(0, 5)
    gather(1, 5)
    gather_end(0)
    gather_end(1)
    for cp in loads[nf:]:
        cp.wait()
    carry = head()
    statistics(carry)
    for ch in range(CHUNKS):
        s0(ch).wait_send()
        for i in (0, 1):
            for j in (0, 1):
                send_fw(ch, i, j).wait_send()
                gf(ch, i, j).wait_send()
            for d in range(n2):
                send_nb(ch, i, d).wait_send()
                gb(ch, i, d).wait_send()
        for d in range(1, n2):
            s2(ch, d).wait_send()
            ga(ch, d).wait_send()
        for d in range(n2):
            for e in range(n2):
                gc(ch, d, e).wait_send()


def final_kernel(lg, stats, out, *rest):
    outs, rows, (buf, sem, row_sem) = rest[:3], rest[3:6], rest[6:]
    vocab = lg.shape[0]
    step = buf.shape[1]
    steps, slots = vocab // step, buf.shape[0]

    def copy(i):
        return pltpu.make_async_copy(buf.at[i % slots], out.at[pl.ds(i * step, step)], sem.at[i % slots])

    for i in range(steps):
        if i >= slots:
            copy(i - slots).wait()
        buf[i % slots] = (lg[pl.ds(i * step, step), :] - stats[0:1, :]).astype(BF16)
        copy(i).start()
        if i == 0:
            small = [pltpu.make_async_copy(rows[j], outs[j], row_sem.at[j]) for j in range(3)]
            for j in range(3):
                rows[j][...] = stats[j, :]
            for cp in small:
                cp.start()
    for cp in small:
        cp.wait()
    for i in range(max(0, steps - slots), steps):
        copy(i).wait()


def solution(mesh):
    model_axes = ('tp2', 'tp')
    n2, n1 = mesh.shape['tp2'], mesh.shape['tp']
    group, nx = n2 * n1, n1 // CORES
    assert nx == n2

    def local_step(hidden, w_gate, w_up, w_down, norm_gain, w_vocab, temperature, target_ids):
        rows, width = hidden.shape
        ff, vocab = w_gate.shape[1], w_vocab.shape[1]
        chunk = rows // CHUNKS
        sl = chunk // group
        half = group // CORES
        hbm, vmem = pl.BlockSpec(memory_space=pl.ANY), pl.BlockSpec(memory_space=pltpu.VMEM)
        dma = pltpu.SemaphoreType.DMA
        c = CHUNKS
        lg, stats = pl.pallas_call(
            lambda *refs: main_kernel(n2, n1, *refs),
            out_shape=(pltpu.VMEM((vocab, rows), F32), pltpu.VMEM((3, rows), F32)),
            in_specs=[hbm] * 9,
            out_specs=(vmem, vmem),
            scratch_shapes=[
                pltpu.VMEM((vocab, width), BF16),
                pltpu.VMEM((c, group, sl, width), BF16),
                pltpu.VMEM((c, half, sl, width), BF16),
                pltpu.VMEM((c, 2, 2, sl, width), BF16),
                pltpu.VMEM((c, 2, n2, sl, width), BF16),
                pltpu.VMEM((c, n2 - 1, sl, width), BF16),
                pltpu.VMEM((c, group, sl, width), BF16),
                pltpu.VMEM((rows, width), BF16),
                pltpu.VMEM((c, sl, width), BF16),
                pltpu.VMEM((rows, ff), BF16),
                pltpu.VMEM((width,), F32),
                pltpu.VMEM((1, rows), F32),
                pltpu.VMEM((1, rows), jnp.int32),
                pltpu.VMEM((HALVES, 4, rows // HALVES), F32),
                pltpu.VMEM((4, rows // HALVES), F32),
                pltpu.VMEM((4, rows // HALVES), F32),
                pltpu.VMEM((half, 4, rows // HALVES), F32),
                pltpu.VMEM((HALVES, 4, rows // HALVES), F32),
                dma((24,)), dma((c,)), dma((3,)), dma((c,)), dma((c,)),
                dma((c, 2, 2)), dma((c, 2, 2)), dma((c, 2, n2)), dma((c, 2, n2)), dma((c, n2 - 1)), dma((c, n2 - 1)),
                dma((c, n2 - 1)), dma((c, 2, n2)), dma((c, 2, 2)), dma((c, n2, n2)), dma((c, group)),
                dma((2,)), dma((2,)), dma((half - 1,)), dma((half,)),
            ],
            name='mlp_head',
            cost_estimate=pl.CostEstimate(flops=2 * rows * width * (vocab + 3 * ff),
                                          bytes_accessed=2 * width * vocab, transcendentals=rows * vocab),
            compiler_params=pltpu.CompilerParams(collective_id=0, has_side_effects=True,
                                                 vmem_limit_bytes=47 * 1024 * 1024),
        )(hidden, hidden.reshape(rows // sl, sl, width), w_gate.T, w_up.T, w_down, norm_gain,
          w_vocab.T, temperature[None, :], target_ids[None, :])
        row = jax.ShapeDtypeStruct((rows,), F32)
        out, *small = pl.pallas_call(
            final_kernel,
            out_shape=(jax.ShapeDtypeStruct((vocab, rows), BF16), row, row, row),
            in_specs=[vmem, vmem],
            out_specs=(hbm,) * 4,
            scratch_shapes=[pltpu.VMEM((rows,), F32)] * 3 + [pltpu.VMEM((4, vocab // 10, rows), BF16), dma((4,)), dma((3,))],
            name='logprobs',
            compiler_params=pltpu.CompilerParams(vmem_limit_bytes=16 * 1024 * 1024),
        )(lg, stats)
        return *small, out.T

    return jax.shard_map(
        local_step, mesh=mesh,
        in_specs=(P('dp', None), P(None, model_axes), P(None, model_axes), P(model_axes, None),
                  P(None), P(None, model_axes), P('dp'), P('dp')),
        out_specs=(P('dp'), P('dp'), P('dp'), P('dp', model_axes)),
        check_vma=False)
```

```python
import functools

import jax
import jax.numpy as jnp
from jax import lax
from jax.experimental import pallas as pl
from jax.experimental.pallas import tpu as pltpu
from jax.sharding import PartitionSpec as P

NORM_EPS = 1e-6
CORES = 2
HALVES = 2
CHUNKS = 2
BLOCKS = 20
UNROLL = 2
UNIT = 32
MESH = pl.DeviceIdType.MESH
NT = (((1,), (1,)), ((), ()))
F32, BF16 = jnp.float32, jnp.bfloat16


def split(start, stop, pieces):
    step = -(-(stop - start) // pieces)
    step = -(-step // 16) * 16
    return [(i, min(step, stop - i)) for i in range(start, stop, step)]


def main_kernel(n2, n1, hid, hid3, wg, wu, wd, gain, wvt, temp, tid, lg, stats,
                wv, yp, d0, fw, nb, st2, xf, xm, hs, act, gain_v, temp_v, tid_v, so, pair_st, chip_st, sr, done,
                load_sem, hs_sem, small_sem, s0_s, s0_r, fw_s, fw_r, nb_s, nb_r, s2_s, s2_r,
                ga_s, gb_s, gf_s, gd_s, gc_s, g_r, sw_s, sw_r, so_s, so_r):
    group = n1 * n2
    half = group // CORES
    rows, width = hid.shape
    ff = wg.shape[0]
    vocab = wvt.shape[0]
    chunk = rows // CHUNKS
    block = vocab // BLOCKS

    y = lax.axis_index('tp2')
    t = lax.axis_index('tp')
    core = lax.rem(t, CORES)
    x = lax.div(t, CORES)
    me = y * n1 + t
    f = y + core * (x - y)
    s = x + core * (y - x)
    mine = core * half + f * n2 + s

    def dev(a, b):
        return {'tp2': a + core * (b - a), 'tp': CORES * (b + core * (a - b)) + core}

    partner = {'tp2': y, 'tp': CORES * x + (1 - core)}

    def slab(a, b):
        return core * half + a * n2 + b

    def remote(src, dst, ssem, rsem, to):
        return pltpu.make_async_remote_copy(src_ref=src, dst_ref=dst, send_sem=ssem, recv_sem=rsem,
                                            device_id=to, device_id_type=MESH)

    right, left, far = (lax.rem(f + i, n2) for i in (1, n2 - 1, 2))
    peers = [dev(right, s), dev(left, s), partner] + [dev(f, lax.rem(s + d, n2)) for d in range(1, n2)]
    barrier = pltpu.get_barrier_semaphore()
    for p in peers:
        pl.semaphore_signal(barrier, inc=1, device_id=p, device_id_type=MESH)

    h0 = vocab - 3 * ff - rows
    g0, d_0 = h0 + rows, h0 + rows + 2 * ff
    quarter = chunk // CORES
    need = [1 - core, core]

    def rows_of(j):
        return [(hid.at[pl.ds(pl.multiple_of(ch * chunk + need[j] * quarter, quarter), quarter)],
                 wv.at[pl.ds(h0 + j * chunk + ch * quarter, quarter)]) for ch in range(CHUNKS)]

    first = [(wg, wv.at[pl.ds(g0, ff)]), (wu, wv.at[pl.ds(g0 + ff, ff)])] + rows_of(0) + rows_of(1)
    first += [(wd, wv.at[pl.ds(d_0, ff)])]
    head_rows = split(0, h0, 9)
    tail_rows = split(h0, vocab, 2)
    loads = [pltpu.make_async_copy(a, b, load_sem.at[i]) for i, (a, b) in enumerate(first)]
    loads += [pltpu.make_async_copy(wvt.at[pl.ds(a, n)], wv.at[pl.ds(a, n)], load_sem.at[len(first) + i])
              for i, (a, n) in enumerate(head_rows + tail_rows)]
    nf, nh = len(first), len(head_rows)
    for cp in loads[:nf]:
        cp.start()
    hcopy = [pltpu.make_async_copy(hid3.at[ch * group + mine], hs.at[ch], hs_sem.at[ch]) for ch in range(CHUNKS)]
    small = [pltpu.make_async_copy(a, b, small_sem.at[i])
             for i, (a, b) in enumerate(((gain, gain_v), (temp, temp_v), (tid, tid_v)))]
    for cp in hcopy + small:
        cp.start()

    def gate_up():
        gu = lax.dot_general(wv[pl.ds(g0, 2 * ff), :], wv[pl.ds(h0, rows), :], NT, preferred_element_type=F32)
        at = jax.nn.silu(gu[:ff]) * gu[ff:]
        act[...] = at.T.astype(BF16)

    def down(j):
        step = 256
        for n in range(width // step):
            cols = pl.ds(n * step, step)
            part = jnp.dot(act[pl.ds(j * chunk, chunk), :], wv[pl.ds(d_0, ff), cols], preferred_element_type=F32)
            yp[:, pl.ds(need[j] * half, half), :, cols] = part.reshape(
                CHUNKS, half, chunk // group, step).astype(BF16)

    def s0(ch):
        return remote(yp.at[ch, pl.ds((1 - core) * half, half)], d0.at[ch], s0_s.at[ch], s0_r.at[ch], partner)

    LATE = ((2, 1), (3, 0))

    def at_s(d):
        return lax.rem(s + d, n2)

    def send_fw(ch, i, j):
        return remote(yp.at[ch, slab(far, at_s(LATE[i][j]))], fw.at[ch, i, j], fw_s.at[ch, i, j],
                      fw_r.at[ch, i, j], dev((right, left)[i], s))

    def send_nb(ch, i, d):
        to = (right, left)[i]
        return remote(yp.at[ch, slab(to, at_s(d))], nb.at[ch, i, d], nb_s.at[ch, i, d],
                      nb_r.at[ch, i, d], dev(to, s))

    def s2(ch, d):
        to = lax.rem(s + d, n2)
        return remote(yp.at[ch, slab(f, to)], st2.at[ch, d - 1], s2_s.at[ch, d - 1],
                      s2_r.at[ch, d - 1], dev(f, to))

    def add0(ch):
        s0(ch).wait_recv()

        def body(i, _):
            k = core * half + i
            yp[ch, k] = (yp[ch, k].astype(F32) + d0[ch, i].astype(F32)).astype(BF16)
            return 0
        lax.fori_loop(0, half, body, 0)

    def send1(ch):
        for j in (0, 1):
            for i in (0, 1):
                send_fw(ch, i, j).start()

    def send1b(ch):
        for j in (0, 1):
            for i in (0, 1):
                send_nb(ch, i, LATE[1 - i][j]).start()

    def pass1(ch):
        for j in (0, 1):
            for i in (0, 1):
                d = LATE[i][j]
                send_fw(ch, i, j).wait_recv()
                k = slab((right, left)[i], at_s(d))
                yp[ch, k] = (yp[ch, k].astype(F32) + fw[ch, i, j].astype(F32)).astype(BF16)
                send_nb(ch, i, d).start()

    def add1(ch):
        for d in (2, 3, 1, 0):
            for i in (0, 1):
                send_nb(ch, i, d).wait_recv()
            k = slab(f, at_s(d))
            yp[ch, k] = (yp[ch, k].astype(F32) + nb[ch, 0, d].astype(F32) + nb[ch, 1, d].astype(F32)).astype(BF16)
            if d:
                s2(ch, d).start()

    def norm(ch):
        for d in range(1, n2):
            s2(ch, d).wait_recv()
        acc = yp[ch, mine].astype(F32)
        for d in range(n2 - 1):
            acc = acc + st2[ch, d].astype(F32)
        r = hs[ch].astype(F32) + acc.astype(BF16).astype(F32)
        inv = lax.rsqrt(jnp.mean(r * r, axis=-1, keepdims=True) + NORM_EPS)
        xf[ch, mine] = (gain_v[...].reshape(1, width) * r * inv).astype(BF16)

    def ga(ch, d):
        ref = xf.at[ch, mine]
        return remote(ref, ref, ga_s.at[ch, d - 1], g_r.at[ch, mine], dev(f, at_s(d)))

    def back(a, e):
        return slab(a, at_s(n2 - e))

    def gb(ch, i, e):
        k = back(f, e)
        ref = xf.at[ch, k]
        return remote(ref, ref, gb_s.at[ch, i, e], g_r.at[ch, k], dev((right, left)[i], s))

    PASS = ((0, 1), (3,))

    def gd(ch):
        ref = xf.at[ch, mine]
        return remote(ref, ref, gd_s.at[ch], g_r.at[ch, mine], dev(far, at_s(2)))

    def gf(ch, i, j):
        k = back((left, right)[i], PASS[i][j])
        ref = xf.at[ch, k]
        return remote(ref, ref, gf_s.at[ch, i, j], g_r.at[ch, k], dev((right, left)[i], s))

    def gc(ch, d, e):
        k = back(lax.rem(f + d, n2), e)
        ref = xf.at[ch, k]
        return remote(ref, ref, gc_s.at[ch, d, e], g_r.at[ch, k], partner)

    def got(ch, k):
        ref = xf.at[ch, k]
        remote(ref, ref, ga_s.at[ch, 0], g_r.at[ch, k], partner).wait_recv()

    def out_own(ch, e):
        if e:
            got(ch, back(f, e))
        for i in (0, 1):
            gb(ch, i, e).start()
        gc(ch, 0, e).start()

    def from_side(ch, e):
        for i in ((0, 1) if e in PASS[0] else (1, 0)):
            got(ch, back((left, right)[i], e))
            if e in PASS[i]:
                gf(ch, i, PASS[i].index(e)).start()
            gc(ch, (n2 - 1, 1)[i], e).start()

    def from_far(ch, e):
        got(ch, back(far, e))
        gc(ch, 2, e).start()

    def gather(ch, part):
        if part == 0:
            for d in (2, 1, 3):
                ga(ch, d).start()
            out_own(ch, 0)
            gd(ch).start()
        elif part == 1:
            out_own(ch, 1)
            out_own(ch, 3)
        elif part == 2:
            from_side(ch, 0)
            out_own(ch, 2)
        elif part == 3:
            from_side(ch, 1)
            from_side(ch, 3)
        elif part == 4:
            from_far(ch, 0)
            from_far(ch, 2)
            from_side(ch, 2)
        else:
            for e in (1, 3):
                from_far(ch, e)

    def gather_end(ch):
        for k in range(half):
            got(ch, (1 - core) * half + k)

        def body(j, _):
            v = xf[ch, pl.ds(2 * j, 2)].astype(F32).reshape(2 * (chunk // group), width)
            xm[pl.ds(pl.multiple_of(ch * chunk + j * 16, 16), 16), :] = v.astype(BF16)
            return 0
        lax.fori_loop(0, group // 2, body, 0)

    def head():
        inv_t = 1.0 / temp_v[...]
        lanes = lax.broadcasted_iota(jnp.int32, (8, rows), 0)
        ids = tid_v[...] - me * vocab - lanes

        def products(i):
            for u in range(UNROLL):
                rs = pl.ds(pl.multiple_of((i * UNROLL + u) * block, 16), block)
                l = lax.dot_general(wv[rs, :], xm[...], NT, preferred_element_type=F32)
                lg[rs, :] = l * inv_t

        def update(i, carry):
            m, total, moment, target = carry
            for u in range(UNROLL):
                base = (i * UNROLL + u) * block
                here = ids - base
                for g in range(0, block, UNIT):
                    n = min(UNIT, block - g)
                    l = lg[pl.ds(pl.multiple_of(base + g, 8), n), :]
                    parts = [l[j:j + 8] for j in range(0, n, 8)]
                    tops = parts
                    while len(tops) > 1:
                        tops = [jnp.maximum(*tops[j:j + 2]) if j + 1 < len(tops) else tops[j]
                                for j in range(0, len(tops), 2)]
                    top = jnp.maximum(m, tops[0])
                    scale = jnp.exp(m - top)
                    total, moment, m = total * scale, moment * scale, top
                    for j, p in enumerate(parts):
                        e = jnp.exp(p - top)
                        total, moment = total + e, moment + e * p
                        target = jnp.where(here == g + 8 * j, p, target)
            return m, total, moment, target

        def body(i, carry):
            carry = update(i - 1, carry)
            products(i)
            return carry

        z = jnp.zeros((8, rows), F32)
        products(0)
        steps = BLOCKS // UNROLL
        carry = lax.fori_loop(1, steps, body, (jnp.full((8, rows), -3.4e38, F32), z, z, z))
        return update(steps - 1, carry)

    chips = group // CORES
    chip = y * (n1 // CORES) + x

    def swap(src, dst, k):
        return remote(src, dst, sw_s.at[k], sw_r.at[k], partner)

    def stat(k):
        i = lax.rem(chip + k, chips)
        to = {'tp2': lax.div(i, n1 // CORES), 'tp': CORES * lax.rem(i, n1 // CORES) + core}
        return remote(chip_st, sr.at[chip], so_s.at[k - 1], so_r.at[chip], to)

    def statistics(carry):
        m8, s8, q8, t8 = carry
        m = jnp.max(m8, axis=0, keepdims=True)
        w = jnp.exp(m8 - m)
        rows4 = [m, jnp.sum(s8 * w, axis=0, keepdims=True), jnp.sum(q8 * w, axis=0, keepdims=True),
                 jnp.sum(t8, axis=0, keepdims=True)]
        for j in range(4):
            for h in range(HALVES):
                so[h, j:j + 1] = rows4[j][:, h * chunk:(h + 1) * chunk]
        first = swap(so.at[1 - core], pair_st, 0)
        first.start()
        first.wait_recv()
        a, b = so[core], pair_st[...]
        m = jnp.maximum(a[0:1], b[0:1])
        wa, wb = jnp.exp(a[0:1] - m), jnp.exp(b[0:1] - m)
        chip_st[0:1] = m
        chip_st[1:3] = a[1:3] * wa + b[1:3] * wb
        chip_st[3:4] = a[3:4] + b[3:4]
        for k in range(1, chips):
            stat(k).start()
        sr[chip] = chip_st[...]
        for k in range(1, chips):
            i = lax.rem(chip + k, chips)
            remote(chip_st, sr.at[i], so_s.at[0], so_r.at[i], partner).wait_recv()
        m = sr[:, 0, :]
        top = jnp.max(m, axis=0, keepdims=True)
        w = jnp.exp(m - top)
        total = jnp.sum(sr[:, 1, :] * w, axis=0, keepdims=True)
        moment = jnp.sum(sr[:, 2, :] * w, axis=0, keepdims=True)
        log_norm = top + jnp.log(total)
        done[core, 0:1] = log_norm
        done[core, 1:2] = log_norm - moment / total
        done[core, 2:3] = jnp.sum(sr[:, 3, :], axis=0, keepdims=True) - log_norm
        second = swap(done.at[core], done.at[core], 1)
        second.start()
        swap(done.at[1 - core], done.at[1 - core], 1).wait_recv()
        for h in range(HALVES):
            stats[:, h * chunk:(h + 1) * chunk] = done[h, 0:3]
        first.wait_send()
        second.wait_send()
        for k in range(1, chips):
            stat(k).wait_send()

    for cp in loads[:nf - 1]:
        cp.wait()
    gate_up()
    loads[nf - 1].wait()
    for cp in loads[nf:nf + nh]:
        cp.start()
    down(0)
    pl.semaphore_wait(barrier, len(peers))
    s0(0).start()
    s0(1).start()
    down(1)
    for cp in loads[nf + nh:]:
        cp.start()
    add0(0)
    send1(0)
    add0(1)
    send1(1)
    send1b(0)
    send1b(1)
    pass1(0)
    pass1(1)
    for cp in hcopy + small:
        cp.wait()
    add1(0)
    add1(1)
    norm(0)
    gather(0, 0)
    norm(1)
    gather(1, 0)
    gather(0, 1)
    gather(1, 1)
    gather(0, 2)
    gather(1, 2)
    gather(0, 3)
    gather(1, 3)
    gather(0, 4)
    gather(1, 4)
    gather(0, 5)
    gather(1, 5)
    gather_end(0)
    gather_end(1)
    for cp in loads[nf:]:
        cp.wait()
    carry = head()
    statistics(carry)
    for ch in range(CHUNKS):
        s0(ch).wait_send()
        for i in (0, 1):
            for j in (0, 1):
                send_fw(ch, i, j).wait_send()
            for j in range(len(PASS[i])):
                gf(ch, i, j).wait_send()
            for d in range(n2):
                send_nb(ch, i, d).wait_send()
                gb(ch, i, d).wait_send()
        gd(ch).wait_send()
        for d in range(1, n2):
            s2(ch, d).wait_send()
            ga(ch, d).wait_send()
        for d in range(n2):
            for e in range(n2):
                gc(ch, d, e).wait_send()


def final_kernel(lg, stats, out, *rest):
    outs, rows, (buf, sem, row_sem) = rest[:3], rest[3:6], rest[6:]
    vocab = lg.shape[0]
    step = buf.shape[1]
    steps, slots = vocab // step, buf.shape[0]

    def copy(i):
        return pltpu.make_async_copy(buf.at[i % slots], out.at[pl.ds(i * step, step)], sem.at[i % slots])

    for i in range(steps):
        if i >= slots:
            copy(i - slots).wait()
        buf[i % slots] = (lg[pl.ds(i * step, step), :] - stats[0:1, :]).astype(BF16)
        copy(i).start()
        if i == 0:
            small = [pltpu.make_async_copy(rows[j], outs[j], row_sem.at[j]) for j in range(3)]
            for j in range(3):
                rows[j][...] = stats[j, :]
            for cp in small:
                cp.start()
    for cp in small:
        cp.wait()
    for i in range(max(0, steps - slots), steps):
        copy(i).wait()


def solution(mesh):
    model_axes = ('tp2', 'tp')
    n2, n1 = mesh.shape['tp2'], mesh.shape['tp']
    group, nx = n2 * n1, n1 // CORES
    assert nx == n2

    def local_step(hidden, w_gate, w_up, w_down, norm_gain, w_vocab, temperature, target_ids):
        rows, width = hidden.shape
        ff, vocab = w_gate.shape[1], w_vocab.shape[1]
        chunk = rows // CHUNKS
        sl = chunk // group
        half = group // CORES
        hbm, vmem = pl.BlockSpec(memory_space=pl.ANY), pl.BlockSpec(memory_space=pltpu.VMEM)
        dma = pltpu.SemaphoreType.DMA
        c = CHUNKS
        lg, stats = pl.pallas_call(
            lambda *refs: main_kernel(n2, n1, *refs),
            out_shape=(pltpu.VMEM((vocab, rows), F32), pltpu.VMEM((3, rows), F32)),
            in_specs=[hbm] * 9,
            out_specs=(vmem, vmem),
            scratch_shapes=[
                pltpu.VMEM((vocab, width), BF16),
                pltpu.VMEM((c, group, sl, width), BF16),
                pltpu.VMEM((c, half, sl, width), BF16),
                pltpu.VMEM((c, 2, 2, sl, width), BF16),
                pltpu.VMEM((c, 2, n2, sl, width), BF16),
                pltpu.VMEM((c, n2 - 1, sl, width), BF16),
                pltpu.VMEM((c, group, sl, width), BF16),
                pltpu.VMEM((rows, width), BF16),
                pltpu.VMEM((c, sl, width), BF16),
                pltpu.VMEM((rows, ff), BF16),
                pltpu.VMEM((width,), F32),
                pltpu.VMEM((1, rows), F32),
                pltpu.VMEM((1, rows), jnp.int32),
                pltpu.VMEM((HALVES, 4, rows // HALVES), F32),
                pltpu.VMEM((4, rows // HALVES), F32),
                pltpu.VMEM((4, rows // HALVES), F32),
                pltpu.VMEM((half, 4, rows // HALVES), F32),
                pltpu.VMEM((HALVES, 4, rows // HALVES), F32),
                dma((24,)), dma((c,)), dma((3,)), dma((c,)), dma((c,)),
                dma((c, 2, 2)), dma((c, 2, 2)), dma((c, 2, n2)), dma((c, 2, n2)), dma((c, n2 - 1)), dma((c, n2 - 1)),
                dma((c, n2 - 1)), dma((c, 2, n2)), dma((c, 2, 2)), dma((c,)), dma((c, n2, n2)), dma((c, group)),
                dma((2,)), dma((2,)), dma((half - 1,)), dma((half,)),
            ],
            name='mlp_head',
            cost_estimate=pl.CostEstimate(flops=2 * rows * width * (vocab + 3 * ff),
                                          bytes_accessed=2 * width * vocab, transcendentals=rows * vocab),
            compiler_params=pltpu.CompilerParams(collective_id=0, has_side_effects=True,
                                                 vmem_limit_bytes=47 * 1024 * 1024),
        )(hidden, hidden.reshape(rows // sl, sl, width), w_gate.T, w_up.T, w_down, norm_gain,
          w_vocab.T, temperature[None, :], target_ids[None, :])
        row = jax.ShapeDtypeStruct((rows,), F32)
        out, *small = pl.pallas_call(
            final_kernel,
            out_shape=(jax.ShapeDtypeStruct((vocab, rows), BF16), row, row, row),
            in_specs=[vmem, vmem],
            out_specs=(hbm,) * 4,
            scratch_shapes=[pltpu.VMEM((rows,), F32)] * 3 + [pltpu.VMEM((4, vocab // 10, rows), BF16), dma((4,)), dma((3,))],
            name='logprobs',
            compiler_params=pltpu.CompilerParams(vmem_limit_bytes=16 * 1024 * 1024),
        )(lg, stats)
        return *small, out.T

    return jax.shard_map(
        local_step, mesh=mesh,
        in_specs=(P('dp', None), P(None, model_axes), P(None, model_axes), P(model_axes, None),
                  P(None), P(None, model_axes), P('dp'), P('dp')),
        out_specs=(P('dp'), P('dp'), P('dp'), P('dp', model_axes)),
        check_vma=False)
```

```python
import functools

import jax
import jax.numpy as jnp
from jax import lax
from jax.experimental import pallas as pl
from jax.experimental.pallas import tpu as pltpu
from jax.sharding import PartitionSpec as P

NORM_EPS = 1e-6
CORES = 2
HALVES = 2
PARTS = 3
CHUNKS = 2
BLOCKS = 20
UNROLL = 2
UNIT = 32
MESH = pl.DeviceIdType.MESH
NT = (((1,), (1,)), ((), ()))
F32, BF16 = jnp.float32, jnp.bfloat16


def split(start, stop, pieces):
    step = -(-(stop - start) // pieces)
    step = -(-step // 16) * 16
    return [(i, min(step, stop - i)) for i in range(start, stop, step)]


def main_kernel(n2, n1, hid, hid3, wg, wu, wd, gain, wvt, temp, tid, lg, stats,
                wv, yp, d0, fw, nb, st2, xf, xm, hs, act, gain_v, temp_v, tid_v, so, pair_st, chip_st, sr, done,
                load_sem, hs_sem, small_sem, s0_s, s0_r, fw_s, fw_r, nb_s, nb_r, s2_s, s2_r,
                ga_s, gb_s, gf_s, gd_s, gs_s, gc_s, g_r, sw_s, sw_r, so_s, so_r):
    group = n1 * n2
    half = group // CORES
    rows, width = hid.shape
    ff = wg.shape[0]
    vocab = wvt.shape[0]
    chunk = rows // CHUNKS
    block = vocab // BLOCKS

    y = lax.axis_index('tp2')
    t = lax.axis_index('tp')
    core = lax.rem(t, CORES)
    x = lax.div(t, CORES)
    me = y * n1 + t
    f = y + core * (x - y)
    s = x + core * (y - x)
    mine = core * half + f * n2 + s

    def dev(a, b):
        return {'tp2': a + core * (b - a), 'tp': CORES * (b + core * (a - b)) + core}

    partner = {'tp2': y, 'tp': CORES * x + (1 - core)}

    def slab(a, b):
        return core * half + a * n2 + b

    def remote(src, dst, ssem, rsem, to):
        return pltpu.make_async_remote_copy(src_ref=src, dst_ref=dst, send_sem=ssem, recv_sem=rsem,
                                            device_id=to, device_id_type=MESH)

    right, left, far = (lax.rem(f + i, n2) for i in (1, n2 - 1, 2))
    peers = [dev(right, s), dev(left, s), partner] + [dev(f, lax.rem(s + d, n2)) for d in range(1, n2)]
    h0 = vocab - 3 * ff - rows
    g0, d_0 = h0 + rows, h0 + rows + 2 * ff
    quarter = chunk // CORES
    need = [1 - core, core]

    def rows_of(j):
        return [(hid.at[pl.ds(pl.multiple_of(ch * chunk + need[j] * quarter, quarter), quarter)],
                 wv.at[pl.ds(h0 + j * chunk + ch * quarter, quarter)]) for ch in range(CHUNKS)]

    first = [(wg, wv.at[pl.ds(g0, ff)]), (wu, wv.at[pl.ds(g0 + ff, ff)])] + rows_of(0) + rows_of(1)
    first += [(wd, wv.at[pl.ds(d_0, ff)])]
    head_rows = split(0, h0, 9)
    tail_rows = split(h0, vocab, 2)
    loads = [pltpu.make_async_copy(a, b, load_sem.at[i]) for i, (a, b) in enumerate(first)]
    loads += [pltpu.make_async_copy(wvt.at[pl.ds(a, n)], wv.at[pl.ds(a, n)], load_sem.at[len(first) + i])
              for i, (a, n) in enumerate(head_rows + tail_rows)]
    nf, nh = len(first), len(head_rows)
    for cp in loads[:nf]:
        cp.start()
    barrier = pltpu.get_barrier_semaphore()
    for p in peers:
        pl.semaphore_signal(barrier, inc=1, device_id=p, device_id_type=MESH)
    hcopy = [pltpu.make_async_copy(hid3.at[ch * group + mine], hs.at[ch], hs_sem.at[ch]) for ch in range(CHUNKS)]
    small = [pltpu.make_async_copy(a, b, small_sem.at[i])
             for i, (a, b) in enumerate(((gain, gain_v), (temp, temp_v), (tid, tid_v)))]
    for cp in hcopy + small:
        cp.start()

    def gate_up():
        gu = lax.dot_general(wv[pl.ds(g0, 2 * ff), :], wv[pl.ds(h0, rows), :], NT, preferred_element_type=F32)
        at = jax.nn.silu(gu[:ff]) * gu[ff:]
        act[...] = at.T.astype(BF16)

    def down(j, after=None):
        step = 256
        for n in range(width // step):
            cols = pl.ds(n * step, step)
            part = jnp.dot(act[pl.ds(j * chunk, chunk), :], wv[pl.ds(d_0, ff), cols], preferred_element_type=F32)
            yp[:, pl.ds(need[j] * half, half), :, cols] = part.reshape(
                CHUNKS, half, chunk // group, step).astype(BF16)
            if after is not None and (n + 1) % (width // step // PARTS) == 0:
                after((n + 1) // (width // step // PARTS) - 1)

    def s0(ch, part):
        cols = pl.ds(part * (width // PARTS), width // PARTS)
        return remote(yp.at[ch, pl.ds((1 - core) * half, half), :, cols], d0.at[ch, :, :, cols],
                      s0_s.at[ch, part], s0_r.at[ch, part], partner)

    LATE = ((2, 1), (3, 0))

    def at_s(d):
        return lax.rem(s + d, n2)

    def send_fw(ch, i, j):
        return remote(yp.at[ch, slab(far, at_s(LATE[i][j]))], fw.at[ch, i, j], fw_s.at[ch, i, j],
                      fw_r.at[ch, i, j], dev((right, left)[i], s))

    def send_nb(ch, i, d):
        to = (right, left)[i]
        return remote(yp.at[ch, slab(to, at_s(d))], nb.at[ch, i, d], nb_s.at[ch, i, d],
                      nb_r.at[ch, i, d], dev(to, s))

    def s2(ch, d):
        to = lax.rem(s + d, n2)
        return remote(yp.at[ch, slab(f, to)], st2.at[ch, d - 1], s2_s.at[ch, d - 1],
                      s2_r.at[ch, d - 1], dev(f, to))

    def add0(ch):
        for part in range(PARTS):
            s0(ch, part).wait_recv()

        def body(i, _):
            k = core * half + i
            yp[ch, k] = (yp[ch, k].astype(F32) + d0[ch, i].astype(F32)).astype(BF16)
            return 0
        lax.fori_loop(0, half, body, 0)

    def send1(ch):
        for j in (0, 1):
            for i in (0, 1):
                send_fw(ch, i, j).start()

    def send1b(ch):
        for j in (0, 1):
            for i in (0, 1):
                send_nb(ch, i, LATE[1 - i][j]).start()

    def pass1(ch):
        for j in (0, 1):
            for i in (0, 1):
                d = LATE[i][j]
                send_fw(ch, i, j).wait_recv()
                k = slab((right, left)[i], at_s(d))
                yp[ch, k] = (yp[ch, k].astype(F32) + fw[ch, i, j].astype(F32)).astype(BF16)
                send_nb(ch, i, d).start()

    def add1(ch):
        for d in (2, 3, 1, 0):
            for i in (0, 1):
                send_nb(ch, i, d).wait_recv()
            k = slab(f, at_s(d))
            yp[ch, k] = (yp[ch, k].astype(F32) + nb[ch, 0, d].astype(F32) + nb[ch, 1, d].astype(F32)).astype(BF16)
            if d:
                s2(ch, d).start()

    def norm(ch):
        for d in range(1, n2):
            s2(ch, d).wait_recv()
        acc = yp[ch, mine].astype(F32)
        for d in range(n2 - 1):
            acc = acc + st2[ch, d].astype(F32)
        r = hs[ch].astype(F32) + acc.astype(BF16).astype(F32)
        inv = lax.rsqrt(jnp.mean(r * r, axis=-1, keepdims=True) + NORM_EPS)
        xf[ch, mine] = (gain_v[...].reshape(1, width) * r * inv).astype(BF16)

    def ga(ch, d):
        ref = xf.at[ch, mine]
        return remote(ref, ref, ga_s.at[ch, d - 1], g_r.at[ch, mine], dev(f, at_s(d)))

    def back(a, e):
        return slab(a, at_s(n2 - e))

    def gb(ch, i, e):
        k = back(f, e)
        ref = xf.at[ch, k]
        return remote(ref, ref, gb_s.at[ch, i, e], g_r.at[ch, k], dev((right, left)[i], s))

    PASS = (((0, 1), (3,)), ((0, 1), ()))
    STRAIGHT = ((), (3,))

    def gs(ch, e):
        k = back(f, e)
        ref = xf.at[ch, k]
        return remote(ref, ref, gs_s.at[ch, e], g_r.at[ch, k], dev(far, s))

    def gd(ch):
        ref = xf.at[ch, mine]
        return remote(ref, ref, gd_s.at[ch], g_r.at[ch, mine], dev(far, at_s(2)))

    def gf(ch, i, j):
        k = back((left, right)[i], PASS[ch][i][j])
        ref = xf.at[ch, k]
        return remote(ref, ref, gf_s.at[ch, i, j], g_r.at[ch, k], dev((right, left)[i], s))

    def gc(ch, d, e):
        k = back(lax.rem(f + d, n2), e)
        ref = xf.at[ch, k]
        return remote(ref, ref, gc_s.at[ch, d, e], g_r.at[ch, k], partner)

    def got(ch, k):
        ref = xf.at[ch, k]
        remote(ref, ref, ga_s.at[ch, 0], g_r.at[ch, k], partner).wait_recv()

    def out_own(ch, e):
        if e:
            got(ch, back(f, e))
        for i in (0, 1):
            gb(ch, i, e).start()
        if e in STRAIGHT[ch]:
            gs(ch, e).start()
        gc(ch, 0, e).start()

    def from_side(ch, e):
        for i in ((0, 1) if e < 2 else (1, 0)):
            got(ch, back((left, right)[i], e))
            if e in PASS[ch][i]:
                gf(ch, i, PASS[ch][i].index(e)).start()
            gc(ch, (n2 - 1, 1)[i], e).start()

    def from_far(ch, e):
        got(ch, back(far, e))
        gc(ch, 2, e).start()

    def gather(ch, part):
        if part == 0:
            for d in (2, 1, 3):
                ga(ch, d).start()
            out_own(ch, 0)
            gd(ch).start()
        elif part == 1:
            out_own(ch, 1)
            out_own(ch, 3)
        elif part == 2:
            from_side(ch, 0)
            out_own(ch, 2)
        elif part == 3:
            from_side(ch, 1)
            from_side(ch, 3)
        elif part == 4:
            from_far(ch, 0)
            from_far(ch, 2)
            from_side(ch, 2)
        else:
            for e in (1, 3):
                from_far(ch, e)

    def gather_end(ch):
        for k in range(half):
            got(ch, (1 - core) * half + k)

        def body(j, _):
            v = xf[ch, pl.ds(2 * j, 2)].astype(F32).reshape(2 * (chunk // group), width)
            xm[pl.ds(pl.multiple_of(ch * chunk + j * 16, 16), 16), :] = v.astype(BF16)
            return 0
        lax.fori_loop(0, group // 2, body, 0)

    def head():
        inv_t = 1.0 / temp_v[...]
        lanes = lax.broadcasted_iota(jnp.int32, (8, rows), 0)
        ids = tid_v[...] - me * vocab - lanes

        def products(i):
            for u in range(UNROLL):
                rs = pl.ds(pl.multiple_of((i * UNROLL + u) * block, 16), block)
                l = lax.dot_general(wv[rs, :], xm[...], NT, preferred_element_type=F32)
                lg[rs, :] = l * inv_t

        def update(i, carry):
            m, total, moment, target = carry
            for u in range(UNROLL):
                base = (i * UNROLL + u) * block
                here = ids - base
                for g in range(0, block, UNIT):
                    n = min(UNIT, block - g)
                    l = lg[pl.ds(pl.multiple_of(base + g, 8), n), :]
                    parts = [l[j:j + 8] for j in range(0, n, 8)]
                    tops = parts
                    while len(tops) > 1:
                        tops = [jnp.maximum(*tops[j:j + 2]) if j + 1 < len(tops) else tops[j]
                                for j in range(0, len(tops), 2)]
                    top = jnp.maximum(m, tops[0])
                    scale = jnp.exp(m - top)
                    total, moment, m = total * scale, moment * scale, top
                    for j, p in enumerate(parts):
                        e = jnp.exp(p - top)
                        total, moment = total + e, moment + e * p
                        target = jnp.where(here == g + 8 * j, p, target)
            return m, total, moment, target

        def body(i, carry):
            carry = update(i - 1, carry)
            products(i)
            return carry

        z = jnp.zeros((8, rows), F32)
        products(0)
        steps = BLOCKS // UNROLL
        carry = lax.fori_loop(1, steps, body, (jnp.full((8, rows), -3.4e38, F32), z, z, z))
        return update(steps - 1, carry)

    chips = group // CORES
    chip = y * (n1 // CORES) + x

    def swap(src, dst, k):
        return remote(src, dst, sw_s.at[k], sw_r.at[k], partner)

    def stat(k):
        i = lax.rem(chip + k, chips)
        to = {'tp2': lax.div(i, n1 // CORES), 'tp': CORES * lax.rem(i, n1 // CORES) + core}
        return remote(chip_st, sr.at[chip], so_s.at[k - 1], so_r.at[chip], to)

    def statistics(carry):
        m8, s8, q8, t8 = carry
        m = jnp.max(m8, axis=0, keepdims=True)
        w = jnp.exp(m8 - m)
        rows4 = [m, jnp.sum(s8 * w, axis=0, keepdims=True), jnp.sum(q8 * w, axis=0, keepdims=True),
                 jnp.sum(t8, axis=0, keepdims=True)]
        for j in range(4):
            for h in range(HALVES):
                so[h, j:j + 1] = rows4[j][:, h * chunk:(h + 1) * chunk]
        first = swap(so.at[1 - core], pair_st, 0)
        first.start()
        first.wait_recv()
        a, b = so[core], pair_st[...]
        m = jnp.maximum(a[0:1], b[0:1])
        wa, wb = jnp.exp(a[0:1] - m), jnp.exp(b[0:1] - m)
        chip_st[0:1] = m
        chip_st[1:3] = a[1:3] * wa + b[1:3] * wb
        chip_st[3:4] = a[3:4] + b[3:4]
        for k in range(1, chips):
            stat(k).start()
        sr[chip] = chip_st[...]
        for k in range(1, chips):
            i = lax.rem(chip + k, chips)
            remote(chip_st, sr.at[i], so_s.at[0], so_r.at[i], partner).wait_recv()
        m = sr[:, 0, :]
        top = jnp.max(m, axis=0, keepdims=True)
        w = jnp.exp(m - top)
        total = jnp.sum(sr[:, 1, :] * w, axis=0, keepdims=True)
        moment = jnp.sum(sr[:, 2, :] * w, axis=0, keepdims=True)
        log_norm = top + jnp.log(total)
        done[core, 0:1] = log_norm
        done[core, 1:2] = log_norm - moment / total
        done[core, 2:3] = jnp.sum(sr[:, 3, :], axis=0, keepdims=True) - log_norm
        second = swap(done.at[core], done.at[core], 1)
        second.start()
        swap(done.at[1 - core], done.at[1 - core], 1).wait_recv()
        for h in range(HALVES):
            stats[:, h * chunk:(h + 1) * chunk] = done[h, 0:3]
        first.wait_send()
        second.wait_send()
        for k in range(1, chips):
            stat(k).wait_send()

    for cp in loads[:nf - 1]:
        cp.wait()
    gate_up()
    loads[nf - 1].wait()
    for cp in loads[nf:nf + nh]:
        cp.start()
    pl.semaphore_wait(barrier, len(peers))
    down(0, lambda part: s0(0, part).start())
    for part in range(PARTS):
        s0(1, part).start()
    down(1)
    for cp in loads[nf + nh:]:
        cp.start()
    add0(0)
    send1(0)
    add0(1)
    send1(1)
    send1b(0)
    send1b(1)
    pass1(0)
    pass1(1)
    for cp in hcopy + small:
        cp.wait()
    add1(0)
    add1(1)
    norm(0)
    gather(0, 0)
    norm(1)
    gather(1, 0)
    gather(0, 1)
    gather(1, 1)
    gather(0, 2)
    gather(1, 2)
    gather(0, 3)
    gather(1, 3)
    gather(0, 4)
    gather(1, 4)
    gather(0, 5)
    gather(1, 5)
    gather_end(0)
    gather_end(1)
    for cp in loads[nf:]:
        cp.wait()
    carry = head()
    statistics(carry)
    for ch in range(CHUNKS):
        for part in range(PARTS):
            s0(ch, part).wait_send()
        for i in (0, 1):
            for j in (0, 1):
                send_fw(ch, i, j).wait_send()
            for j in range(len(PASS[ch][i])):
                gf(ch, i, j).wait_send()
            for d in range(n2):
                send_nb(ch, i, d).wait_send()
                gb(ch, i, d).wait_send()
        gd(ch).wait_send()
        for e in STRAIGHT[ch]:
            gs(ch, e).wait_send()
        for d in range(1, n2):
            s2(ch, d).wait_send()
            ga(ch, d).wait_send()
        for d in range(n2):
            for e in range(n2):
                gc(ch, d, e).wait_send()


def final_kernel(lg, stats, out, *rest):
    outs, rows, (buf, sem, row_sem) = rest[:3], rest[3:6], rest[6:]
    vocab = lg.shape[0]
    step, slots = buf.shape[1], buf.shape[0]
    sizes = [step // 2] + [step] * (vocab // step - 1) + [step // 2]
    starts = [sum(sizes[:i]) for i in range(len(sizes))]
    steps = len(sizes)

    def copy(i):
        return pltpu.make_async_copy(buf.at[i % slots, pl.ds(0, sizes[i])], out.at[pl.ds(starts[i], sizes[i])],
                                     sem.at[i % slots])

    for i in range(steps):
        if i >= slots:
            copy(i - slots).wait()
        buf[i % slots, 0:sizes[i]] = (lg[pl.ds(starts[i], sizes[i]), :] - stats[0:1, :]).astype(BF16)
        copy(i).start()
        if i == 0:
            small = [pltpu.make_async_copy(rows[j], outs[j], row_sem.at[j]) for j in range(3)]
            for j in range(3):
                rows[j][...] = stats[j, :]
            for cp in small:
                cp.start()
    for cp in small:
        cp.wait()
    for i in range(max(0, steps - slots), steps):
        copy(i).wait()


def solution(mesh):
    model_axes = ('tp2', 'tp')
    n2, n1 = mesh.shape['tp2'], mesh.shape['tp']
    group, nx = n2 * n1, n1 // CORES
    assert nx == n2

    def local_step(hidden, w_gate, w_up, w_down, norm_gain, w_vocab, temperature, target_ids):
        rows, width = hidden.shape
        ff, vocab = w_gate.shape[1], w_vocab.shape[1]
        chunk = rows // CHUNKS
        sl = chunk // group
        half = group // CORES
        hbm, vmem = pl.BlockSpec(memory_space=pl.ANY), pl.BlockSpec(memory_space=pltpu.VMEM)
        dma = pltpu.SemaphoreType.DMA
        c = CHUNKS
        lg, stats = pl.pallas_call(
            lambda *refs: main_kernel(n2, n1, *refs),
            out_shape=(pltpu.VMEM((vocab, rows), F32), pltpu.VMEM((3, rows), F32)),
            in_specs=[hbm] * 9,
            out_specs=(vmem, vmem),
            scratch_shapes=[
                pltpu.VMEM((vocab, width), BF16),
                pltpu.VMEM((c, group, sl, width), BF16),
                pltpu.VMEM((c, half, sl, width), BF16),
                pltpu.VMEM((c, 2, 2, sl, width), BF16),
                pltpu.VMEM((c, 2, n2, sl, width), BF16),
                pltpu.VMEM((c, n2 - 1, sl, width), BF16),
                pltpu.VMEM((c, group, sl, width), BF16),
                pltpu.VMEM((rows, width), BF16),
                pltpu.VMEM((c, sl, width), BF16),
                pltpu.VMEM((rows, ff), BF16),
                pltpu.VMEM((width,), F32),
                pltpu.VMEM((1, rows), F32),
                pltpu.VMEM((1, rows), jnp.int32),
                pltpu.VMEM((HALVES, 4, rows // HALVES), F32),
                pltpu.VMEM((4, rows // HALVES), F32),
                pltpu.VMEM((4, rows // HALVES), F32),
                pltpu.VMEM((half, 4, rows // HALVES), F32),
                pltpu.VMEM((HALVES, 4, rows // HALVES), F32),
                dma((24,)), dma((c,)), dma((3,)), dma((c, PARTS)), dma((c, PARTS)),
                dma((c, 2, 2)), dma((c, 2, 2)), dma((c, 2, n2)), dma((c, 2, n2)), dma((c, n2 - 1)), dma((c, n2 - 1)),
                dma((c, n2 - 1)), dma((c, 2, n2)), dma((c, 2, 2)), dma((c,)), dma((c, n2)), dma((c, n2, n2)), dma((c, group)),
                dma((2,)), dma((2,)), dma((half - 1,)), dma((half,)),
            ],
            name='mlp_head',
            cost_estimate=pl.CostEstimate(flops=2 * rows * width * (vocab + 3 * ff),
                                          bytes_accessed=2 * width * vocab, transcendentals=rows * vocab),
            compiler_params=pltpu.CompilerParams(collective_id=0, has_side_effects=True,
                                                 vmem_limit_bytes=47 * 1024 * 1024),
        )(hidden, hidden.reshape(rows // sl, sl, width), w_gate.T, w_up.T, w_down, norm_gain,
          w_vocab.T, temperature[None, :], target_ids[None, :])
        row = jax.ShapeDtypeStruct((rows,), F32)
        out, *small = pl.pallas_call(
            final_kernel,
            out_shape=(jax.ShapeDtypeStruct((vocab, rows), BF16), row, row, row),
            in_specs=[vmem, vmem],
            out_specs=(hbm,) * 4,
            scratch_shapes=[pltpu.VMEM((rows,), F32)] * 3 + [pltpu.VMEM((4, vocab // 10, rows), BF16), dma((4,)), dma((3,))],
            name='logprobs',
            compiler_params=pltpu.CompilerParams(vmem_limit_bytes=16 * 1024 * 1024),
        )(lg, stats)
        return *small, out.T

    return jax.shard_map(
        local_step, mesh=mesh,
        in_specs=(P('dp', None), P(None, model_axes), P(None, model_axes), P(model_axes, None),
                  P(None), P(None, model_axes), P('dp'), P('dp')),
        out_specs=(P('dp'), P('dp'), P('dp'), P('dp', model_axes)),
        check_vma=False)
```

```python
import functools

import jax
import jax.numpy as jnp
from jax import lax
from jax.experimental import pallas as pl
from jax.experimental.pallas import tpu as pltpu
from jax.sharding import PartitionSpec as P

NORM_EPS = 1e-6
CORES = 2
HALVES = 2
PARTS = 3
CHUNKS = 2
BLOCKS = 20
UNROLL = 2
UNIT = 32
MESH = pl.DeviceIdType.MESH
NT = (((1,), (1,)), ((), ()))
F32, BF16 = jnp.float32, jnp.bfloat16


def split(start, stop, pieces):
    step = -(-(stop - start) // pieces)
    step = -(-step // 16) * 16
    return [(i, min(step, stop - i)) for i in range(start, stop, step)]


def main_kernel(n2, n1, hid, hid3, wg, wu, wd, gain, wvt, temp, tid, lg, stats,
                wv, yp, d0, fw, nb, st2, xf, xm, hs, act, gain_v, temp_v, tid_v, so, sr, done,
                load_sem, hs_sem, small_sem, s0_s, s0_r, fw_s, fw_r, nb_s, nb_r, s2_s, s2_r,
                ga_s, gb_s, gf_s, gd_s, gs_s, gc_s, g_r, sw_s, sw_r, so_s, so_r):
    group = n1 * n2
    half = group // CORES
    rows, width = hid.shape
    ff = wg.shape[0]
    vocab = wvt.shape[0]
    chunk = rows // CHUNKS
    block = vocab // BLOCKS

    y = lax.axis_index('tp2')
    t = lax.axis_index('tp')
    core = lax.rem(t, CORES)
    x = lax.div(t, CORES)
    me = y * n1 + t
    f = y + core * (x - y)
    s = x + core * (y - x)
    mine = core * half + f * n2 + s

    def dev(a, b):
        return {'tp2': a + core * (b - a), 'tp': CORES * (b + core * (a - b)) + core}

    partner = {'tp2': y, 'tp': CORES * x + (1 - core)}

    def slab(a, b):
        return core * half + a * n2 + b

    def remote(src, dst, ssem, rsem, to):
        return pltpu.make_async_remote_copy(src_ref=src, dst_ref=dst, send_sem=ssem, recv_sem=rsem,
                                            device_id=to, device_id_type=MESH)

    right, left, far = (lax.rem(f + i, n2) for i in (1, n2 - 1, 2))
    peers = [dev(right, s), dev(left, s), partner] + [dev(f, lax.rem(s + d, n2)) for d in range(1, n2)]
    h0 = vocab - 3 * ff - rows
    g0, d_0 = h0 + rows, h0 + rows + 2 * ff
    quarter = chunk // CORES
    need = [1 - core, core]

    def rows_of(j):
        return [(hid.at[pl.ds(pl.multiple_of(ch * chunk + need[j] * quarter, quarter), quarter)],
                 wv.at[pl.ds(h0 + j * chunk + ch * quarter, quarter)]) for ch in range(CHUNKS)]

    first = [(wg, wv.at[pl.ds(g0, ff)]), (wu, wv.at[pl.ds(g0 + ff, ff)])] + rows_of(0) + rows_of(1)
    first += [(wd, wv.at[pl.ds(d_0, ff)])]
    head_rows = split(0, h0, 9)
    tail_rows = split(h0, vocab, 2)
    loads = [pltpu.make_async_copy(a, b, load_sem.at[i]) for i, (a, b) in enumerate(first)]
    loads += [pltpu.make_async_copy(wvt.at[pl.ds(a, n)], wv.at[pl.ds(a, n)], load_sem.at[len(first) + i])
              for i, (a, n) in enumerate(head_rows + tail_rows)]
    nf, nh = len(first), len(head_rows)
    for cp in loads[:nf]:
        cp.start()
    barrier = pltpu.get_barrier_semaphore()
    for p in peers:
        pl.semaphore_signal(barrier, inc=1, device_id=p, device_id_type=MESH)
    hcopy = [pltpu.make_async_copy(hid3.at[ch * group + mine], hs.at[ch], hs_sem.at[ch]) for ch in range(CHUNKS)]
    small = [pltpu.make_async_copy(a, b, small_sem.at[i])
             for i, (a, b) in enumerate(((gain, gain_v), (temp, temp_v), (tid, tid_v)))]
    for cp in hcopy + small:
        cp.start()

    def gate_up():
        gu = lax.dot_general(wv[pl.ds(g0, 2 * ff), :], wv[pl.ds(h0, rows), :], NT, preferred_element_type=F32)
        at = jax.nn.silu(gu[:ff]) * gu[ff:]
        act[...] = at.T.astype(BF16)

    def down(j, after=None):
        step = 256
        for n in range(width // step):
            cols = pl.ds(n * step, step)
            part = jnp.dot(act[pl.ds(j * chunk, chunk), :], wv[pl.ds(d_0, ff), cols], preferred_element_type=F32)
            yp[:, pl.ds(need[j] * half, half), :, cols] = part.reshape(
                CHUNKS, half, chunk // group, step).astype(BF16)
            if after is not None and (n + 1) % (width // step // PARTS) == 0:
                after((n + 1) // (width // step // PARTS) - 1)

    def s0(ch, part):
        cols = pl.ds(part * (width // PARTS), width // PARTS)
        return remote(yp.at[ch, pl.ds((1 - core) * half, half), :, cols], d0.at[ch, :, :, cols],
                      s0_s.at[ch, part], s0_r.at[ch, part], partner)

    LATE = ((2, 1), (3, 0))

    def at_s(d):
        return lax.rem(s + d, n2)

    def send_fw(ch, i, j):
        return remote(yp.at[ch, slab(far, at_s(LATE[i][j]))], fw.at[ch, i, j], fw_s.at[ch, i, j],
                      fw_r.at[ch, i, j], dev((right, left)[i], s))

    def send_nb(ch, i, d):
        to = (right, left)[i]
        return remote(yp.at[ch, slab(to, at_s(d))], nb.at[ch, i, d], nb_s.at[ch, i, d],
                      nb_r.at[ch, i, d], dev(to, s))

    def s2(ch, d):
        to = lax.rem(s + d, n2)
        return remote(yp.at[ch, slab(f, to)], st2.at[ch, d - 1], s2_s.at[ch, d - 1],
                      s2_r.at[ch, d - 1], dev(f, to))

    def add0(ch):
        for part in range(PARTS):
            s0(ch, part).wait_recv()

        def body(i, _):
            k = core * half + i
            yp[ch, k] = (yp[ch, k].astype(F32) + d0[ch, i].astype(F32)).astype(BF16)
            return 0
        lax.fori_loop(0, half, body, 0)

    def send1(ch):
        for j in (0, 1):
            for i in (0, 1):
                send_fw(ch, i, j).start()

    def send1b(ch):
        for j in (0, 1):
            for i in (0, 1):
                send_nb(ch, i, LATE[1 - i][j]).start()

    def pass1(ch):
        for j in (0, 1):
            for i in (0, 1):
                d = LATE[i][j]
                send_fw(ch, i, j).wait_recv()
                k = slab((right, left)[i], at_s(d))
                yp[ch, k] = (yp[ch, k].astype(F32) + fw[ch, i, j].astype(F32)).astype(BF16)
                send_nb(ch, i, d).start()

    def add1(ch):
        for d in (2, 3, 1, 0):
            for i in (0, 1):
                send_nb(ch, i, d).wait_recv()
            k = slab(f, at_s(d))
            yp[ch, k] = (yp[ch, k].astype(F32) + nb[ch, 0, d].astype(F32) + nb[ch, 1, d].astype(F32)).astype(BF16)
            if d:
                s2(ch, d).start()

    def norm(ch):
        for d in range(1, n2):
            s2(ch, d).wait_recv()
        acc = yp[ch, mine].astype(F32)
        for d in range(n2 - 1):
            acc = acc + st2[ch, d].astype(F32)
        r = hs[ch].astype(F32) + acc.astype(BF16).astype(F32)
        inv = lax.rsqrt(jnp.mean(r * r, axis=-1, keepdims=True) + NORM_EPS)
        xf[ch, mine] = (gain_v[...].reshape(1, width) * r * inv).astype(BF16)

    def ga(ch, d):
        ref = xf.at[ch, mine]
        return remote(ref, ref, ga_s.at[ch, d - 1], g_r.at[ch, mine], dev(f, at_s(d)))

    def back(a, e):
        return slab(a, at_s(n2 - e))

    def gb(ch, i, e):
        k = back(f, e)
        ref = xf.at[ch, k]
        return remote(ref, ref, gb_s.at[ch, i, e], g_r.at[ch, k], dev((right, left)[i], s))

    PASS = (((0, 1), (3,)), ((0, 1), ()))
    STRAIGHT = ((), (3,))

    def gs(ch, e):
        k = back(f, e)
        ref = xf.at[ch, k]
        return remote(ref, ref, gs_s.at[ch, e], g_r.at[ch, k], dev(far, s))

    def gd(ch):
        ref = xf.at[ch, mine]
        return remote(ref, ref, gd_s.at[ch], g_r.at[ch, mine], dev(far, at_s(2)))

    def gf(ch, i, j):
        k = back((left, right)[i], PASS[ch][i][j])
        ref = xf.at[ch, k]
        return remote(ref, ref, gf_s.at[ch, i, j], g_r.at[ch, k], dev((right, left)[i], s))

    def gc(ch, d, e):
        k = back(lax.rem(f + d, n2), e)
        ref = xf.at[ch, k]
        return remote(ref, ref, gc_s.at[ch, d, e], g_r.at[ch, k], partner)

    def got(ch, k):
        ref = xf.at[ch, k]
        remote(ref, ref, ga_s.at[ch, 0], g_r.at[ch, k], partner).wait_recv()

    def out_own(ch, e):
        if e:
            got(ch, back(f, e))
        for i in (0, 1):
            gb(ch, i, e).start()
        if e in STRAIGHT[ch]:
            gs(ch, e).start()
        gc(ch, 0, e).start()

    def from_side(ch, e):
        for i in ((0, 1) if e < 2 else (1, 0)):
            got(ch, back((left, right)[i], e))
            if e in PASS[ch][i]:
                gf(ch, i, PASS[ch][i].index(e)).start()
            gc(ch, (n2 - 1, 1)[i], e).start()

    def from_far(ch, e):
        got(ch, back(far, e))
        gc(ch, 2, e).start()

    def gather(ch, part):
        if part == 0:
            for d in (2, 1, 3):
                ga(ch, d).start()
            out_own(ch, 0)
            gd(ch).start()
        elif part == 1:
            out_own(ch, 1)
            out_own(ch, 3)
        elif part == 2:
            from_side(ch, 0)
            out_own(ch, 2)
        elif part == 3:
            from_side(ch, 1)
            from_side(ch, 3)
        elif part == 4:
            from_far(ch, 0)
            from_side(ch, 2)
        else:
            for e in (1, 3, 2):
                from_far(ch, e)

    def gather_end(ch):
        for k in range(half):
            got(ch, (1 - core) * half + k)

        def body(j, _):
            v = xf[ch, pl.ds(2 * j, 2)].astype(F32).reshape(2 * (chunk // group), width)
            xm[pl.ds(pl.multiple_of(ch * chunk + j * 16, 16), 16), :] = v.astype(BF16)
            return 0
        lax.fori_loop(0, group // 2, body, 0)

    def head():
        inv_t = 1.0 / temp_v[...]
        lanes = lax.broadcasted_iota(jnp.int32, (8, rows), 0)
        ids = tid_v[...] - me * vocab - lanes

        def products(i):
            for u in range(UNROLL):
                rs = pl.ds(pl.multiple_of((i * UNROLL + u) * block, 16), block)
                l = lax.dot_general(wv[rs, :], xm[...], NT, preferred_element_type=F32)
                lg[rs, :] = l * inv_t

        def update(i, carry):
            m, total, moment, target = carry
            for u in range(UNROLL):
                base = (i * UNROLL + u) * block
                here = ids - base
                for g in range(0, block, UNIT):
                    n = min(UNIT, block - g)
                    l = lg[pl.ds(pl.multiple_of(base + g, 8), n), :]
                    parts = [l[j:j + 8] for j in range(0, n, 8)]
                    tops = parts
                    while len(tops) > 1:
                        tops = [jnp.maximum(*tops[j:j + 2]) if j + 1 < len(tops) else tops[j]
                                for j in range(0, len(tops), 2)]
                    top = jnp.maximum(m, tops[0])
                    scale = jnp.exp(m - top)
                    total, moment, m = total * scale, moment * scale, top
                    for j, p in enumerate(parts):
                        e = jnp.exp(p - top)
                        total, moment = total + e, moment + e * p
                        target = jnp.where(here == g + 8 * j, p, target)
            return m, total, moment, target

        def body(i, carry):
            carry = update(i - 1, carry)
            products(i)
            return carry

        z = jnp.zeros((8, rows), F32)
        products(0)
        steps = BLOCKS // UNROLL
        carry = lax.fori_loop(1, steps, body, (jnp.full((8, rows), -3.4e38, F32), z, z, z))
        return update(steps - 1, carry)

    chips = group // CORES

    def swap(src, dst, k):
        return remote(src, dst, sw_s.at[k], sw_r.at[k], partner)

    nx = n1 // CORES
    others = sorted(((a, b) for a in range(n2) for b in range(nx) if a or b),
                    key=lambda o: -min(o[0], n2 - o[0]) - min(o[1], nx - o[1]))

    def other_chip(k):
        a, b = others[k - 1]
        return lax.rem(y + a, n2), lax.rem(x + b, nx)

    def stat(k, same):
        a, b = other_chip(k) if k else (y, x)
        to = core if same else 1 - core
        return remote(so.at[to], sr.at[me], so_s.at[same, k], so_r.at[me], {'tp2': a, 'tp': CORES * b + to})

    def stat_from(k, same):
        a, b = other_chip(k) if k else (y, x)
        i = a * n1 + CORES * b + (core if same else 1 - core)
        return remote(so.at[0], sr.at[i], so_s.at[same, k], so_r.at[i], partner)

    targets = [(k, same) for k in range(1, chips) for same in (0, 1)] + [(0, 0)]

    def statistics(carry):
        m8, s8, q8, t8 = carry
        m = jnp.max(m8, axis=0, keepdims=True)
        w = jnp.exp(m8 - m)
        rows4 = [m, jnp.sum(s8 * w, axis=0, keepdims=True), jnp.sum(q8 * w, axis=0, keepdims=True),
                 jnp.sum(t8, axis=0, keepdims=True)]
        for j in range(4):
            for h in range(HALVES):
                so[h, j:j + 1] = rows4[j][:, h * chunk:(h + 1) * chunk]
        for k, same in targets:
            stat(k, same).start()
        sr[me] = so[core]
        for k, same in targets:
            stat_from(k, same).wait_recv()
        m = sr[:, 0, :]
        top = jnp.max(m, axis=0, keepdims=True)
        w = jnp.exp(m - top)
        total = jnp.sum(sr[:, 1, :] * w, axis=0, keepdims=True)
        moment = jnp.sum(sr[:, 2, :] * w, axis=0, keepdims=True)
        log_norm = top + jnp.log(total)
        done[core, 0:1] = log_norm
        done[core, 1:2] = log_norm - moment / total
        done[core, 2:3] = jnp.sum(sr[:, 3, :], axis=0, keepdims=True) - log_norm
        second = swap(done.at[core], done.at[core], 0)
        second.start()
        swap(done.at[1 - core], done.at[1 - core], 0).wait_recv()
        for h in range(HALVES):
            stats[:, h * chunk:(h + 1) * chunk] = done[h, 0:3]
        second.wait_send()
        for k, same in targets:
            stat(k, same).wait_send()

    for cp in loads[:nf - 1]:
        cp.wait()
    gate_up()
    loads[nf - 1].wait()
    for cp in loads[nf:nf + nh]:
        cp.start()
    pl.semaphore_wait(barrier, len(peers))
    down(0, lambda part: s0(0, part).start())
    for part in range(PARTS):
        s0(1, part).start()
    down(1)
    for cp in loads[nf + nh:]:
        cp.start()
    add0(0)
    send1(0)
    add0(1)
    send1(1)
    send1b(0)
    send1b(1)
    pass1(0)
    pass1(1)
    for cp in hcopy + small:
        cp.wait()
    add1(0)
    add1(1)
    norm(0)
    gather(0, 0)
    norm(1)
    gather(1, 0)
    gather(0, 1)
    gather(1, 1)
    gather(0, 2)
    gather(1, 2)
    gather(0, 3)
    gather(1, 3)
    gather(0, 4)
    gather(1, 4)
    gather(0, 5)
    gather(1, 5)
    gather_end(0)
    gather_end(1)
    for cp in loads[nf:]:
        cp.wait()
    carry = head()
    statistics(carry)
    for ch in range(CHUNKS):
        for part in range(PARTS):
            s0(ch, part).wait_send()
        for i in (0, 1):
            for j in (0, 1):
                send_fw(ch, i, j).wait_send()
            for j in range(len(PASS[ch][i])):
                gf(ch, i, j).wait_send()
            for d in range(n2):
                send_nb(ch, i, d).wait_send()
                gb(ch, i, d).wait_send()
        gd(ch).wait_send()
        for e in STRAIGHT[ch]:
            gs(ch, e).wait_send()
        for d in range(1, n2):
            s2(ch, d).wait_send()
            ga(ch, d).wait_send()
        for d in range(n2):
            for e in range(n2):
                gc(ch, d, e).wait_send()


def final_kernel(lg, stats, out, *rest):
    outs, rows, (buf, sem, row_sem) = rest[:3], rest[3:6], rest[6:]
    vocab = lg.shape[0]
    step, slots = buf.shape[1], buf.shape[0]
    sizes = [step // 2] + [step] * (vocab // step - 1) + [step // 2]
    starts = [sum(sizes[:i]) for i in range(len(sizes))]
    steps = len(sizes)

    def copy(i):
        return pltpu.make_async_copy(buf.at[i % slots, pl.ds(0, sizes[i])], out.at[pl.ds(starts[i], sizes[i])],
                                     sem.at[i % slots])

    for i in range(steps):
        if i >= slots:
            copy(i - slots).wait()
        buf[i % slots, 0:sizes[i]] = (lg[pl.ds(starts[i], sizes[i]), :] - stats[0:1, :]).astype(BF16)
        copy(i).start()
        if i == 0:
            small = [pltpu.make_async_copy(rows[j], outs[j], row_sem.at[j]) for j in range(3)]
            for j in range(3):
                rows[j][...] = stats[j, :]
            for cp in small:
                cp.start()
    for cp in small:
        cp.wait()
    for i in range(max(0, steps - slots), steps):
        copy(i).wait()


def solution(mesh):
    model_axes = ('tp2', 'tp')
    n2, n1 = mesh.shape['tp2'], mesh.shape['tp']
    group, nx = n2 * n1, n1 // CORES
    assert nx == n2

    def local_step(hidden, w_gate, w_up, w_down, norm_gain, w_vocab, temperature, target_ids):
        rows, width = hidden.shape
        ff, vocab = w_gate.shape[1], w_vocab.shape[1]
        chunk = rows // CHUNKS
        sl = chunk // group
        half = group // CORES
        hbm, vmem = pl.BlockSpec(memory_space=pl.ANY), pl.BlockSpec(memory_space=pltpu.VMEM)
        dma = pltpu.SemaphoreType.DMA
        c = CHUNKS
        lg, stats = pl.pallas_call(
            lambda *refs: main_kernel(n2, n1, *refs),
            out_shape=(pltpu.VMEM((vocab, rows), F32), pltpu.VMEM((3, rows), F32)),
            in_specs=[hbm] * 9,
            out_specs=(vmem, vmem),
            scratch_shapes=[
                pltpu.VMEM((vocab, width), BF16),
                pltpu.VMEM((c, group, sl, width), BF16),
                pltpu.VMEM((c, half, sl, width), BF16),
                pltpu.VMEM((c, 2, 2, sl, width), BF16),
                pltpu.VMEM((c, 2, n2, sl, width), BF16),
                pltpu.VMEM((c, n2 - 1, sl, width), BF16),
                pltpu.VMEM((c, group, sl, width), BF16),
                pltpu.VMEM((rows, width), BF16),
                pltpu.VMEM((c, sl, width), BF16),
                pltpu.VMEM((rows, ff), BF16),
                pltpu.VMEM((width,), F32),
                pltpu.VMEM((1, rows), F32),
                pltpu.VMEM((1, rows), jnp.int32),
                pltpu.VMEM((HALVES, 4, rows // HALVES), F32),
                pltpu.VMEM((group, 4, rows // HALVES), F32),
                pltpu.VMEM((HALVES, 4, rows // HALVES), F32),
                dma((24,)), dma((c,)), dma((3,)), dma((c, PARTS)), dma((c, PARTS)),
                dma((c, 2, 2)), dma((c, 2, 2)), dma((c, 2, n2)), dma((c, 2, n2)), dma((c, n2 - 1)), dma((c, n2 - 1)),
                dma((c, n2 - 1)), dma((c, 2, n2)), dma((c, 2, 2)), dma((c,)), dma((c, n2)), dma((c, n2, n2)), dma((c, group)),
                dma((1,)), dma((1,)), dma((2, half)), dma((group,)),
            ],
            name='mlp_head',
            cost_estimate=pl.CostEstimate(flops=2 * rows * width * (vocab + 3 * ff),
                                          bytes_accessed=2 * width * vocab, transcendentals=rows * vocab),
            compiler_params=pltpu.CompilerParams(collective_id=0, has_side_effects=True,
                                                 vmem_limit_bytes=47 * 1024 * 1024),
        )(hidden, hidden.reshape(rows // sl, sl, width), w_gate.T, w_up.T, w_down, norm_gain,
          w_vocab.T, temperature[None, :], target_ids[None, :])
        row = jax.ShapeDtypeStruct((rows,), F32)
        out, *small = pl.pallas_call(
            final_kernel,
            out_shape=(jax.ShapeDtypeStruct((vocab, rows), BF16), row, row, row),
            in_specs=[vmem, vmem],
            out_specs=(hbm,) * 4,
            scratch_shapes=[pltpu.VMEM((rows,), F32)] * 3 + [pltpu.VMEM((4, vocab // 10, rows), BF16), dma((4,)), dma((3,))],
            name='logprobs',
            compiler_params=pltpu.CompilerParams(vmem_limit_bytes=16 * 1024 * 1024),
        )(lg, stats)
        return *small, out.T

    return jax.shard_map(
        local_step, mesh=mesh,
        in_specs=(P('dp', None), P(None, model_axes), P(None, model_axes), P(model_axes, None),
                  P(None), P(None, model_axes), P('dp'), P('dp')),
        out_specs=(P('dp'), P('dp'), P('dp'), P('dp', model_axes)),
        check_vma=False)
```
